16 devices in a mesh: data: 16 (over z, y, x, core).
Axes of the slice: x: 2, y: 2, z: 2, core: 2. Of those that a mesh axis runs over, the one named last changes fastest.
Arguments:
- x_act: bfloat16 [64, 256, 1024], P('data')
- y_tgt: bfloat16 [64, 256, 1024], P('data')
- w_in: float32 [4, 1024, 4096], P(None, 'data')
- w_out: float32 [4, 4096, 1024], P(None, 'data')
Outputs:
- output 1: float32 [4, 1024, 4096], P(None, 'data')
- output 2: float32 [4, 4096, 1024], P(None, 'data')
- output 3: float32 [], replicated
All inputs are finite; a program needn't handle non-finite values.
Results may differ from the reference program's by a relative error of at most 0.00156061.
Values are sent between devices in bfloat16 or wider.
A program may use at most 1 GiB of HBM per device.

```python
import math
import jax
import jax.numpy as jnp
from jax import lax

LAYERS = 4
IMAGES = 4
PATCHES = 256
WIDTH = 1024
MLP_DIM = 4096
GROUP = 16

TOKENS = IMAGES * PATCHES
RHO_FRAC = 0.1
LEARN_RATE = 0.5
RADIUS = RHO_FRAC * math.sqrt(LAYERS * WIDTH)


def setup_inputs(seed: int = 0) -> dict:
    root_key = jax.random.key(seed)
    k_x, k_y, k_in, k_out = jax.random.split(root_key, 4)
    shape_tok = (GROUP * IMAGES, PATCHES, WIDTH)
    x_act = jax.random.normal(k_x, shape_tok, jnp.float32)
    y_tgt = jax.random.normal(k_y, shape_tok, jnp.float32)
    w_in = jax.random.normal(k_in, (LAYERS, WIDTH, MLP_DIM), jnp.float32) * WIDTH ** -0.5
    w_out = jax.random.normal(k_out, (LAYERS, MLP_DIM, WIDTH), jnp.float32) * (2 * LAYERS * MLP_DIM) ** -0.5
    return {'x_act': x_act.astype(jnp.bfloat16), 'y_tgt': y_tgt.astype(jnp.bfloat16), 'w_in': w_in, 'w_out': w_out}


def gelu_exact(values):
    return jax.nn.gelu(values, approximate=False)


def local_grads(x_tok, y_tok, w_in_b, w_out_b):
    def fwd_step(h_prev, weights):
        w_in_l, w_out_l = weights
        z_pre = jnp.dot(h_prev, w_in_l, preferred_element_type=jnp.float32).astype(jnp.bfloat16)
        gelu_out = gelu_exact(z_pre.astype(jnp.float32)).astype(jnp.bfloat16)
        branch = jnp.dot(gelu_out, w_out_l, preferred_element_type=jnp.float32)
        h_next = (h_prev.astype(jnp.float32) + branch).astype(jnp.bfloat16)
        return h_next, (h_prev, z_pre, gelu_out)

    h_last, saved = lax.scan(fwd_step, x_tok, (w_in_b, w_out_b))
    residual = h_last.astype(jnp.float32) - y_tok.astype(jnp.float32)
    local_loss = 0.5 * jnp.sum(residual * residual) / TOKENS

    def bwd_step(d_res, items):
        h_prev, z_pre, gelu_out, w_in_l, w_out_l = items
        d_bf = d_res.astype(jnp.bfloat16)
        g_out = jnp.dot(gelu_out.T, d_bf, preferred_element_type=jnp.float32)
        d_gelu = jnp.dot(d_bf, w_out_l.T, preferred_element_type=jnp.float32)
        _, gelu_vjp = jax.vjp(gelu_exact, z_pre.astype(jnp.float32))
        d_pre = gelu_vjp(d_gelu)[0].astype(jnp.bfloat16)
        g_in = jnp.dot(h_prev.T, d_pre, preferred_element_type=jnp.float32)
        d_prev = d_res + jnp.dot(d_pre, w_in_l.T, preferred_element_type=jnp.float32)
        return d_prev, (g_in, g_out)

    _, (g_in, g_out) = lax.scan(bwd_step, residual / TOKENS, saved + (w_in_b, w_out_b), reverse=True)
    return local_loss, g_in, g_out


def mean_grads(x_act, y_tgt, w_in_b, w_out_b):
    x_dev = x_act.reshape(GROUP, TOKENS, WIDTH)
    y_dev = y_tgt.reshape(GROUP, TOKENS, WIDTH)

    def add_device(carry, pair):
        loss_sum, sum_in, sum_out = carry
        local_loss, g_in, g_out = local_grads(pair[0], pair[1], w_in_b, w_out_b)
        sum_in = sum_in + g_in.astype(jnp.bfloat16).astype(jnp.float32)
        sum_out = sum_out + g_out.astype(jnp.bfloat16).astype(jnp.float32)
        return (loss_sum + local_loss, sum_in, sum_out), None

    start_carry = (jnp.zeros((), jnp.float32), jnp.zeros((LAYERS, WIDTH, MLP_DIM), jnp.float32), jnp.zeros((LAYERS, MLP_DIM, WIDTH), jnp.float32))
    (loss_sum, sum_in, sum_out), _ = lax.scan(add_device, start_carry, (x_dev, y_dev))
    return loss_sum / GROUP, sum_in / GROUP, sum_out / GROUP


def reference(x_act, y_tgt, w_in, w_out):
    _, g_in, g_out = mean_grads(x_act, y_tgt, w_in.astype(jnp.bfloat16), w_out.astype(jnp.bfloat16))
    grad_norm = jnp.sqrt(jnp.sum(g_in * g_in) + jnp.sum(g_out * g_out))
    scale_eps = RADIUS / grad_norm
    pert_in = (w_in + scale_eps * g_in).astype(jnp.bfloat16)
    pert_out = (w_out + scale_eps * g_out).astype(jnp.bfloat16)
    pert_loss, gp_in, gp_out = mean_grads(x_act, y_tgt, pert_in, pert_out)
    return (w_in - LEARN_RATE * gp_in, w_out - LEARN_RATE * gp_out, pert_loss)
```

```python
import functools
import math
import jax
import jax.numpy as jnp
from jax import lax
from jax.experimental import pallas as pl
from jax.experimental.pallas import tpu as pltpu
from jax.sharding import PartitionSpec as P

RHO_FRAC = 0.1
LEARN_RATE = 0.5
BF = jnp.bfloat16
F32 = jnp.float32
MESH = pl.DeviceIdType.MESH
SQRT_HALF = math.sqrt(0.5)
DENSITY = 1.0 / math.sqrt(2.0 * math.pi)
VMEM_LIMIT = 63 * 2 ** 20
NT = (((1,), (1,)), ((), ()))
CORE, AX_X, AX_Y, AX_Z = 1, 2, 4, 8
COLOR_ORDERS = ((AX_X, AX_Y, AX_Z), (AX_Y, AX_Z, AX_X), (AX_Z, AX_X, AX_Y))
ANY = pl.BlockSpec(memory_space=pl.ANY)


def flip(dev, bit):
    return dev + bit * (1 - 2 * ((dev // bit) % 2))


def flips(dev, mask):
    for bit in (1, 2, 4, 8):
        if mask & bit:
            dev = flip(dev, bit)
    return dev


def greet_neighbours():
    me = lax.axis_index('data')
    barrier = pltpu.get_barrier_semaphore()
    for bit in (CORE, AX_X, AX_Y, AX_Z):
        pl.semaphore_signal(barrier, inc=1, device_id=(flip(me, bit),), device_id_type=MESH)
    pl.semaphore_wait(barrier, 4)


class Gather:
    def __init__(self, shard, full, pieces, recv, send, own_vmem, own_sem):
        self.shard, self.full, self.pieces = shard, full, pieces
        self.recv, self.send = recv, send
        self.own_vmem, self.own_sem = own_vmem, own_sem
        self.me = lax.axis_index('data')

    def piece(self, origin_mask, color):
        rows, cols = self.pieces[color]
        if origin_mask == 0:
            return self.shard.at[rows, cols]
        return self.full.at[flips(self.me, origin_mask), rows, cols]

    def push(self, origin_mask, color, bit, sem_index, send_index):
        rows, cols = self.pieces[color]
        pltpu.make_async_remote_copy(
            src_ref=self.piece(origin_mask, color),
            dst_ref=self.full.at[flips(self.me, origin_mask), rows, cols],
            send_sem=self.send.at[send_index], recv_sem=self.recv.at[sem_index],
            device_id=(flip(self.me, bit),), device_id_type=MESH).start()

    def masks(self, color, stage):
        d1, d2, d3 = COLOR_ORDERS[color]
        return ((0,), (0, d1), (0, d1, d2, d1 | d2))[stage]

    def start(self, stage):
        for color in range(3):
            for mask in self.masks(color, stage):
                self.push(mask, color, COLOR_ORDERS[color][stage], 3 * color + stage, 0)

    def wait(self, stage):
        for color in range(3):
            rows, cols = self.pieces[color]
            landed = self.full.at[pl.ds(0, 2 ** stage), rows, cols]
            pltpu.make_async_copy(landed, landed, self.recv.at[3 * color + stage]).wait()

    def share(self, stage):
        for color in range(3):
            if stage < 0:
                self.push(0, color, CORE, 9, 1)
            else:
                bit = COLOR_ORDERS[color][stage]
                for mask in self.masks(color, stage):
                    self.push(mask | bit, color, CORE, 9, 1)

    def own_load(self):
        pltpu.make_async_copy(self.shard, self.own_vmem, self.own_sem).start()

    def own_store(self):
        pltpu.make_async_copy(self.shard, self.own_vmem, self.own_sem).wait()
        pltpu.make_async_copy(self.own_vmem, self.full.at[self.me], self.own_sem).start()

    def finish(self):
        half = self.full.at[pl.ds(0, 8)]
        pltpu.make_async_copy(half, half, self.recv.at[9]).wait()
        pltpu.make_async_copy(half, half, self.send.at[1]).wait()
        sent = self.full.at[pl.ds(0, 7)]
        pltpu.make_async_copy(sent, sent, self.send.at[0]).wait()
        pltpu.make_async_copy(self.own_vmem, self.full.at[self.me], self.own_sem).wait()


def gather_scratch(sh_in, sh_out):
    return [pltpu.SemaphoreType.DMA((10,)), pltpu.SemaphoreType.DMA((2,)),
            pltpu.SemaphoreType.DMA((10,)), pltpu.SemaphoreType.DMA((2,)),
            pltpu.VMEM(sh_in, BF), pltpu.SemaphoreType.DMA,
            pltpu.VMEM(sh_out, BF), pltpu.SemaphoreType.DMA]


def make_gathers(shard_in, shard_out, full_in, full_out, scratch):
    rin, sin, rout, sout, vin, semin, vout, semout = scratch
    every = slice(None)
    cols = full_in.shape[2]
    tiles = cols // 128
    a = 128 * ((tiles + 2) // 3)
    pieces_in = [(every, pl.ds(0, a)), (every, pl.ds(a, a)), (every, pl.ds(2 * a, cols - 2 * a))]
    rows = full_out.shape[1]
    b = 16 * (rows // 48)
    pieces_out = [(pl.ds(0, b), every), (pl.ds(b, b), every), (pl.ds(2 * b, rows - 2 * b), every)]
    return (Gather(shard_in, full_in, pieces_in, rin, sin, vin, semin),
            Gather(shard_out, full_out, pieces_out, rout, sout, vout, semout))


def gather_kernel(shard_in, shard_out, full_in, full_out, *scratch):
    g_in, g_out = make_gathers(shard_in, shard_out, full_in, full_out, scratch)
    greet_neighbours()
    g_in.start(0)
    g_out.start(0)
    g_in.own_load()
    g_out.own_load()
    g_in.share(-1)
    g_out.share(-1)
    g_in.own_store()
    g_out.own_store()
    for stage in (0, 1, 2):
        for g in (g_in, g_out):
            g.wait(stage)
            if stage < 2:
                g.start(stage + 1)
            g.share(stage)
    g_in.finish()
    g_out.finish()


def gather_layer(shard_in, shard_out):
    return pl.pallas_call(
        gather_kernel,
        out_shape=[jax.ShapeDtypeStruct((16,) + shard_in.shape, BF), jax.ShapeDtypeStruct((16,) + shard_out.shape, BF)],
        in_specs=[ANY, ANY], out_specs=[ANY, ANY],
        scratch_shapes=gather_scratch(shard_in.shape, shard_out.shape),
        compiler_params=pltpu.CompilerParams(collective_id=0, has_side_effects=True, vmem_limit_bytes=VMEM_LIMIT),
        name='gather_first')(shard_in, shard_out)


HB = 512
MT = 512


def gelu_and_slope(z):
    phi = 0.5 + 0.5 * lax.erf(z * SQRT_HALF)
    density = jnp.exp(z * z * -0.5) * DENSITY
    return z * phi, phi + z * density


def forward_compute(step, n_up, h_ref, wi_ref, wo_vmem, d_ref, hn_ref, a_vmem, a_hbm, a_sem):
    tokens = h_ref.shape[0]

    @pl.when(step < n_up)
    def _():
        base = pl.multiple_of(jnp.minimum(step, n_up - 1) * HB, HB)
        for m in range(tokens // MT):
            rows = pl.ds(m * MT, MT)
            z = jnp.dot(h_ref[rows, :], wi_ref[...], preferred_element_type=F32)
            act, slope = gelu_and_slope(z.astype(BF).astype(F32))
            a_vmem[rows, pl.ds(base, HB)] = act.astype(BF)
            d_ref[rows, :] = slope
        pltpu.make_async_copy(a_vmem.at[:, pl.ds(base, HB)], a_hbm.at[:, pl.ds(base, HB)], a_sem).start()

    @pl.when(step >= n_up)
    def _():
        base = pl.multiple_of(jnp.maximum(step - n_up, 0) * MT, MT)
        branch = jnp.dot(a_vmem[pl.ds(base, MT), :], wo_vmem[...], preferred_element_type=F32)
        hn_ref[...] = (h_ref[pl.ds(base, MT), :].astype(F32) + branch).astype(BF)


def forward_kernel(gathering, n_up, n_down, h_ref, wi_ref, wo_hbm, *refs):
    if gathering:
        shard_in, shard_out, a_hbm, d_ref, hn_ref, full_in, full_out, a_vmem, wo_vmem, a_sem, wo_sem, *scratch = refs
        g_in, g_out = make_gathers(shard_in, shard_out, full_in, full_out, scratch)
    else:
        a_hbm, d_ref, hn_ref, a_vmem, wo_vmem, a_sem, wo_sem = refs
    step = pl.program_id(0)

    def at(s, fn):
        pl.when(step == s)(fn)

    def begin():
        pltpu.make_async_copy(wo_hbm, wo_vmem, wo_sem).start()
        if gathering:
            greet_neighbours()
            g_in.start(0)
            g_out.start(0)
            g_in.own_load()
            g_out.own_load()
            g_in.share(-1)
            g_out.share(-1)

    def advance(g, stage):
        def fn():
            g.wait(stage)
            if stage < 2:
                g.start(stage + 1)
            g.share(stage)
        return fn

    at(0, begin)
    if gathering:
        def stores():
            g_in.own_store()
            g_out.own_store()
        at(1, stores)
        at(3, advance(g_in, 0))
        at(4, advance(g_out, 0))
        at(6, advance(g_in, 1))
        at(8, advance(g_out, 1))
        at(11, advance(g_in, 2))
    at(n_up, lambda: pltpu.make_async_copy(wo_hbm, wo_vmem, wo_sem).wait())
    forward_compute(step, n_up, h_ref, wi_ref, wo_vmem, d_ref, hn_ref, a_vmem, a_hbm, a_sem)

    def end():
        pltpu.make_async_copy(a_vmem, a_hbm, a_sem).wait()
        if gathering:
            advance(g_out, 2)()
            g_in.finish()
            g_out.finish()
    at(n_up + n_down - 1, end)


def forward_layer(h, w_in_full, w_out_full, next_shards):
    tokens, width = h.shape
    hidden = w_in_full.shape[1]
    n_up, n_down = hidden // HB, tokens // MT
    gathering = next_shards is not None
    up = lambda s: jnp.minimum(s, n_up - 1)
    down = lambda s: jnp.maximum(s - n_up, 0)
    in_specs = [pl.BlockSpec((tokens, width), lambda s: (0, 0), pipeline_mode=pl.Buffered(1)),
                pl.BlockSpec((width, HB), lambda s: (0, up(s))), ANY]
    out_specs = [ANY, pl.BlockSpec((tokens, HB), lambda s: (0, up(s))), pl.BlockSpec((MT, width), lambda s: (down(s), 0))]
    out_shape = [jax.ShapeDtypeStruct((tokens, hidden), BF), jax.ShapeDtypeStruct((tokens, hidden), F32),
                 jax.ShapeDtypeStruct((tokens, width), BF)]
    scratch = [pltpu.VMEM((tokens, hidden), BF), pltpu.VMEM((hidden, width), BF),
               pltpu.SemaphoreType.DMA, pltpu.SemaphoreType.DMA]
    args = [h, w_in_full, w_out_full]
    params = dict(vmem_limit_bytes=VMEM_LIMIT)
    if gathering:
        sh_in, sh_out = next_shards
        args += [sh_in, sh_out]
        in_specs += [ANY, ANY]
        out_specs += [ANY, ANY]
        out_shape += [jax.ShapeDtypeStruct((16,) + sh_in.shape, BF), jax.ShapeDtypeStruct((16,) + sh_out.shape, BF)]
        scratch += gather_scratch(sh_in.shape, sh_out.shape)
        params.update(collective_id=1, has_side_effects=True)
    return pl.pallas_call(
        functools.partial(forward_kernel, gathering, n_up, n_down), grid=(n_up + n_down,),
        in_specs=in_specs, out_specs=out_specs, out_shape=out_shape, scratch_shapes=scratch,
        compiler_params=pltpu.CompilerParams(**params),
        cost_estimate=pl.CostEstimate(flops=4 * tokens * width * hidden, bytes_accessed=70 * 2 ** 20, transcendentals=0),
        name='forward_gather' if gathering else 'forward_last')(*args)


NB = 256
CHIP_ORDER = (1, 2, 4, 0, 3, 5, 6, 7)
OWNERS = (1, 2, 4, 0)


def pick(index, values):
    out = values[0]
    for i in range(1, len(values)):
        out = jnp.where(index == i, values[i], out)
    return out


def chip_at(turn):
    chip = lax.axis_index('data') // 2
    mask = pick(turn, CHIP_ORDER)
    for bit in (1, 2, 4):
        chip = jnp.where((mask // bit) % 2 == 1, flip(chip, bit), chip)
    return chip


def block_at(step):
    core = lax.axis_index('data') % 2
    return 2 * chip_at(step // 2) + jnp.where(step % 2 == 0, 1 - core, core)


def rounded_sum(lhs_t, rhs, half):
    first = jnp.dot(lhs_t[:, :half], rhs[:half, :], preferred_element_type=F32).astype(BF).astype(F32)
    second = jnp.dot(lhs_t[:, half:], rhs[half:, :], preferred_element_type=F32).astype(BF).astype(F32)
    return first + second


def backward_kernel(with_input_grad, n_in, n_rows, rb_ref, wo_ref, a_ref, d_ref, h_hbm, *refs):
    if with_input_grad:
        wi_ref, r_ref, rn_ref, rbn_ref, gi_out, go_out, *scratch = refs
    else:
        gi_out, go_out, *scratch = refs
    (rbt, ht, hraw, e_ref, gi_x, gi_send, gi_recv, go_x, go_send, go_recv,
     h_sem, dsend, drecv, xsend, xrecv, own_sem) = scratch
    step = pl.program_id(0)
    me = lax.axis_index('data')
    core = me % 2
    tokens, width = rb_ref.shape
    half = tokens // 2
    rows_dev = ht.shape[0] // 8
    mine = 4 * rows_dev
    n_steps = 16
    partner = (flip(me, CORE),)

    def at(s, fn):
        pl.when(step == s)(fn)

    def h_copy(i):
        chip = me // 2
        if OWNERS[i]:
            chip = flip(chip, OWNERS[i])
        cols = pl.multiple_of(chip * 2 * rows_dev, 2 * rows_dev)
        return pltpu.make_async_copy(h_hbm.at[:, pl.ds(cols, 2 * rows_dev)], hraw.at[:, pl.ds(i * 2 * rows_dev, 2 * rows_dev)], h_sem)

    def begin():
        for i in range(4):
            h_copy(i).start()
        greet_neighbours()
        for m in range(tokens // 256):
            rbt[:, pl.ds(m * 256, 256)] = rb_ref[pl.ds(m * 256, 256), :].T

    def turn_h():
        pltpu.make_async_copy(hraw, hraw, h_sem).wait()
        for m in range(tokens // 256):
            cols = pl.ds(m * 256, 256)
            for i in range(4):
                flipped = hraw[pl.ds(m * 256, 256), pl.ds(i * 2 * rows_dev, 2 * rows_dev)].T
                ht[pl.ds(pl.multiple_of(i * rows_dev + core * mine, rows_dev), rows_dev), cols] = flipped[:rows_dev]
                ht[pl.ds(pl.multiple_of(i * rows_dev + (1 - core) * mine, rows_dev), rows_dev), cols] = flipped[rows_dev:]

    def core_copy(src, dst, index):
        return pltpu.make_async_remote_copy(src_ref=src, dst_ref=dst, send_sem=dsend.at[index], recv_sem=drecv.at[index],
                                            device_id=partner, device_id_type=MESH)

    def gi_core(turn):
        return core_copy(gi_send.at[turn % 2], gi_recv.at[turn % 2], turn % 2)

    def go_core(turn):
        return core_copy(go_send.at[turn % 2], go_recv.at[turn % 2], 2 + turn % 2)

    def ship(src, dst, i, kind):
        bit = 2 * OWNERS[i]
        if bit:
            pltpu.make_async_remote_copy(src_ref=src, dst_ref=dst(1 + i), send_sem=xsend.at[3 * kind + i],
                                         recv_sem=xrecv.at[3 * kind + i], device_id=(flip(me, bit),), device_id_type=MESH).start()
        else:
            pltpu.make_async_copy(src, dst(0), own_sem.at[kind]).start()

    def go_merge(turn):
        go_core(turn).wait_recv()
        go_x[turn] = go_x[turn] + go_recv[turn % 2]
        ship(go_x.at[turn], lambda slot: go_out.at[slot], turn, 1)

    def gi_merge(turn):
        gi_core(turn).wait_recv()
        gi_x[turn] = gi_x[turn] + gi_recv[turn % 2]
        cols = pl.ds(pl.multiple_of(chip_at(turn) * 2 * NB, 2 * NB), 2 * NB)
        for i in range(4):
            ship(gi_x.at[turn, pl.ds(i * rows_dev, rows_dev)], lambda slot: gi_out.at[slot, :, cols], i, 0)

    def in_grad(s):
        base = pl.multiple_of(block_at(s) * NB, NB)
        lane = pl.multiple_of(jnp.where(s % 2 == 0, 1 - core, core) * NB, NB)
        turn = s // 2
        total = rounded_sum(ht[...], e_ref[:, pl.ds(base, NB)], half)
        gi_x[turn, :, pl.ds(lane, NB)] = total[:mine]
        gi_send[turn % 2, :, pl.ds(lane, NB)] = total[mine:]

    even = step % 2 == 0
    at(0, begin)
    at(1, turn_h)
    for turn in range(4):
        at(2 * turn + 2, functools.partial(go_merge, turn))
    last_merge = n_steps + 2 if with_input_grad else n_steps
    pl.when(even & (step >= 4) & (step <= last_merge))(lambda: gi_merge(jnp.clip(step // 2 - 2, 0, 7)))
    pl.when((step % 2 == 1) & (step >= 5) & (step < n_steps))(lambda: gi_core(step // 2).wait_send())
    pl.when(even & (step >= 4) & (step < 8))(lambda: go_core(step // 2).wait_send())

    @pl.when(step < n_steps)
    def _():
        base = pl.multiple_of(block_at(jnp.minimum(step, n_steps - 1)) * NB, NB)
        for m in range(tokens // 512):
            rows = pl.ds(m * 512, 512)
            u = lax.dot_general(rb_ref[rows, :], wo_ref[...], NT, preferred_element_type=F32)
            e_ref[rows, pl.ds(base, NB)] = (d_ref[rows, :] * u).astype(BF)

    @pl.when((step >= 1) & (step <= n_steps))
    def _():
        in_grad(jnp.clip(step - 1, 0, n_steps - 1))

    pl.when(even & (step >= 2) & (step <= n_steps))(lambda: gi_core(jnp.maximum(step // 2 - 1, 0)).start())

    @pl.when(step < 8)
    def _():
        turn = jnp.minimum(step // 2, 3)
        for m in range(width // 512):
            rows = pl.ds(m * 512, 512)
            total = rounded_sum(rbt[rows, :], a_ref[...], half)

            @pl.when(even)
            def _():
                go_send[turn % 2, rows, :] = total

            @pl.when(jnp.logical_not(even))
            def _():
                go_x[turn, rows, :] = total

        @pl.when(even)
        def _():
            go_core(turn).start()

    if with_input_grad:
        @pl.when(step >= n_steps)
        def _():
            base = pl.multiple_of((jnp.maximum(step - n_steps, 0) % 2) * half, half)
            for m in range(half // 512):
                rows = pl.ds(m * 512, 512)
                u = lax.dot_general(e_ref[pl.ds(base + m * 512, 512), :], wi_ref[...], NT, preferred_element_type=F32) + r_ref[rows, :]
                rn_ref[rows, :] = u
                rbn_ref[rows, :] = u.astype(BF)

    def end():
        if not with_input_grad:
            gi_merge(7)
        for turn in (6, 7):
            gi_core(turn).wait_send()
        for turn in (2, 3):
            go_core(turn).wait_send()
        for i in range(3):
            for kind, whole in ((0, gi_out.at[0]), (1, go_out.at[0])):
                pltpu.make_async_copy(whole, whole, xsend.at[3 * kind + i]).wait()
                pltpu.make_async_copy(whole, whole, xrecv.at[3 * kind + i]).wait()
        pltpu.make_async_copy(gi_out.at[0], gi_out.at[0], own_sem.at[0]).wait()
        pltpu.make_async_copy(go_out.at[0], go_out.at[0], own_sem.at[1]).wait()
    at(n_steps + (8 if with_input_grad else 1) - 1, end)


def backward_layer(rb, r, h, w_in_full, w_out_full, a, d, with_input_grad):
    tokens, width = rb.shape
    hidden = a.shape[1]
    half = tokens // 2
    rows_dev = width // 16
    cap = lambda s: jnp.minimum(s, 15)
    tail = lambda s: jnp.maximum(s - 16, 0)
    in_specs = [pl.BlockSpec((tokens, width), lambda s: (0, 0), pipeline_mode=pl.Buffered(1)),
                pl.BlockSpec((NB, width), lambda s: (block_at(cap(s)), 0)),
                pl.BlockSpec((tokens, NB), lambda s: (0, block_at(jnp.minimum(s, 7)))),
                pl.BlockSpec((tokens, NB), lambda s: (0, block_at(cap(s)))),
                ANY]
    args = [rb, w_out_full, a, d, h]
    out_specs, out_shape = [], []
    if with_input_grad:
        in_specs += [pl.BlockSpec((NB, hidden), lambda s: (tail(s) // 2, 0)),
                     pl.BlockSpec((half, NB), lambda s: (tail(s) % 2, tail(s) // 2))]
        args += [w_in_full, r]
        out_specs += [pl.BlockSpec((half, NB), lambda s: (tail(s) % 2, tail(s) // 2))] * 2
        out_shape += [jax.ShapeDtypeStruct((tokens, width), F32), jax.ShapeDtypeStruct((tokens, width), BF)]
    out_specs += [ANY, ANY]
    out_shape += [jax.ShapeDtypeStruct((4, rows_dev, hidden), F32), jax.ShapeDtypeStruct((4, width, hidden // 16), F32)]
    scratch = [pltpu.VMEM((width, tokens), BF), pltpu.VMEM((8 * rows_dev, tokens), BF), pltpu.VMEM((tokens, 8 * rows_dev), BF),
               pltpu.VMEM((tokens, hidden), BF),
               pltpu.VMEM((8, 4 * rows_dev, 2 * NB), F32), pltpu.VMEM((2, 4 * rows_dev, 2 * NB), F32), pltpu.VMEM((2, 4 * rows_dev, 2 * NB), F32),
               pltpu.VMEM((4, width, NB), F32), pltpu.VMEM((2, width, NB), F32), pltpu.VMEM((2, width, NB), F32),
               pltpu.SemaphoreType.DMA, pltpu.SemaphoreType.DMA((4,)), pltpu.SemaphoreType.DMA((4,)),
               pltpu.SemaphoreType.DMA((6,)), pltpu.SemaphoreType.DMA((6,)), pltpu.SemaphoreType.DMA((2,))]
    return pl.pallas_call(
        functools.partial(backward_kernel, with_input_grad, 0, rows_dev), grid=(24 if with_input_grad else 17,),
        in_specs=in_specs, out_specs=out_specs, out_shape=out_shape, scratch_shapes=scratch,
        compiler_params=pltpu.CompilerParams(collective_id=2 if with_input_grad else 3, has_side_effects=True, vmem_limit_bytes=VMEM_LIMIT),
        cost_estimate=pl.CostEstimate(flops=6 * tokens * width * hidden, bytes_accessed=100 * 2 ** 20, transcendentals=0),
        name='backward' if with_input_grad else 'backward_first')(*args)


def antipodal(values):
    return lax.ppermute(values, 'data', [(i, i ^ 14) for i in range(16)])


def sam_pass(x_pair, y_pair, shards_in, shards_out):
    layers = len(shards_in)
    own = x_pair.shape[0] // 2
    h_cur = x_pair
    saved = []
    full = gather_layer(shards_in[0], shards_out[0])
    for layer in range(layers):
        w_in_full = full[0].reshape(-1, full[0].shape[-1])
        w_out_full = full[1].reshape(-1, full[1].shape[-1])
        nxt = (shards_in[layer + 1], shards_out[layer + 1]) if layer + 1 < layers else None
        act, slope, h_next, *full = forward_layer(h_cur, w_in_full, w_out_full, nxt)
        saved.append((h_cur, act, slope, w_in_full, w_out_full))
        h_cur = h_next
    residual = h_cur.astype(F32) - y_pair.astype(F32)
    local_loss = 0.5 * jnp.sum(residual[:own] * residual[:own]) / own
    r = residual / own
    rb = r.astype(BF)
    g_in = [None] * layers
    g_out = [None] * layers
    for layer in reversed(range(layers)):
        h_prev, act, slope, w_in_full, w_out_full = saved[layer]
        res = backward_layer(rb, r, h_prev, w_in_full, w_out_full, act, slope, layer > 0)
        if layer > 0:
            r, rb = res[0], res[1]
        g_in[layer] = jnp.sum(res[-2], axis=0) / 16
        g_out[layer] = (jnp.sum(res[-1], axis=0) / 16).T
    return local_loss, g_in, g_out


def solution(mesh):
    groups = mesh.shape['data']

    def device_step(x_blk, y_blk, w_in_sh, w_out_sh):
        layers = w_in_sh.shape[0]
        model_dim = w_out_sh.shape[2]
        radius = RHO_FRAC * math.sqrt(layers * model_dim)
        x_tok = x_blk.reshape(-1, model_dim)
        y_tok = y_blk.reshape(-1, model_dim)
        x_pair = jnp.concatenate([x_tok, antipodal(x_tok)])
        y_pair = jnp.concatenate([y_tok, antipodal(y_tok)])
        span = range(layers)
        _, g_in, g_out = sam_pass(x_pair, y_pair, [w_in_sh[l].astype(BF) for l in span], [w_out_sh[l].astype(BF) for l in span])
        part_sq = sum(jnp.sum(g * g) for g in g_in) + sum(jnp.sum(g * g) for g in g_out)
        grad_norm = jnp.sqrt(lax.psum(part_sq, 'data'))
        scale_eps = radius / grad_norm
        pert_in = [(w_in_sh[l] + scale_eps * g_in[l]).astype(BF) for l in span]
        pert_out = [(w_out_sh[l] + scale_eps * g_out[l]).astype(BF) for l in span]
        pert_loss, gp_in, gp_out = sam_pass(x_pair, y_pair, pert_in, pert_out)
        mean_loss = lax.psum(pert_loss, 'data') / groups
        return w_in_sh - LEARN_RATE * jnp.stack(gp_in), w_out_sh - LEARN_RATE * jnp.stack(gp_out), mean_loss

    return jax.shard_map(device_step, mesh=mesh,
                         in_specs=(P('data', None, None), P('data', None, None), P(None, 'data', None), P(None, 'data', None)),
                         out_specs=(P(None, 'data', None), P(None, 'data', None), P()),
                         check_vma=False)
```

```python
import functools
import math
import jax
import jax.numpy as jnp
from jax import lax
from jax.experimental import pallas as pl
from jax.experimental.pallas import tpu as pltpu
from jax.sharding import PartitionSpec as P

RHO_FRAC = 0.1
LEARN_RATE = 0.5
BF = jnp.bfloat16
F32 = jnp.float32
MESH = pl.DeviceIdType.MESH
DEVICES = 16
LANES = 128
SUM_TILE = (8, LANES)
SQRT_HALF = math.sqrt(0.5)
LOG2_E = math.log2(math.e)
LOG_DENSITY = -0.5 * math.log2(2.0 * math.pi)
VMEM_LIMIT = 63 * 2 ** 20
NT = (((1,), (1,)), ((), ()))
CORE, AX_X, AX_Y, AX_Z = 1, 2, 4, 8
ANTIPODE = AX_X | AX_Y | AX_Z
COLOR_ORDERS = ((AX_X, AX_Y, AX_Z), (AX_Y, AX_Z, AX_X), (AX_Z, AX_X, AX_Y))
ANY = pl.BlockSpec(memory_space=pl.ANY)


def span(index, size):
    return pl.ds(index * size, size)


def flip(dev, bit):
    return dev ^ bit


def flips(dev, mask):
    return dev ^ mask


def greet_neighbours(*more):
    me = lax.axis_index('data')
    barrier = pltpu.get_barrier_semaphore()
    masks = (CORE, AX_X, AX_Y, AX_Z) + more
    for mask in masks:
        pl.semaphore_signal(barrier, inc=1, device_id=(flips(me, mask),), device_id_type=MESH)
    pl.semaphore_wait(barrier, len(masks))


def greet_all():
    me = lax.axis_index('data')
    barrier = pltpu.get_barrier_semaphore()
    for other in range(1, DEVICES):
        pl.semaphore_signal(barrier, inc=1, device_id=((me + other) % DEVICES,), device_id_type=MESH)


def send_to_all(tiles, send, recv):
    me = lax.axis_index('data')
    pl.semaphore_wait(pltpu.get_barrier_semaphore(), DEVICES - 1)
    for other in range(1, DEVICES):
        pltpu.make_async_remote_copy(src_ref=tiles.at[me], dst_ref=tiles.at[me], send_sem=send, recv_sem=recv,
                                     device_id=((me + other) % DEVICES,), device_id_type=MESH).start()


def sum_of_all(tiles, send, recv):
    others = tiles.at[pl.ds(0, DEVICES - 1)]
    pltpu.make_async_copy(others, others, recv).wait()
    pltpu.make_async_copy(others, others, send).wait()
    return jnp.sum(tiles[...], axis=0)


TILE_SCRATCH = [pltpu.VMEM((DEVICES,) + SUM_TILE, F32), pltpu.SemaphoreType.DMA, pltpu.SemaphoreType.DMA]


class Gather:
    def __init__(self, full, pieces, sems, shard=None, own_vmem=None, own_sem=None):
        self.shard, self.full, self.pieces = shard, full, pieces
        self.recv, self.send = sems
        self.own_vmem, self.own_sem = own_vmem, own_sem
        self.me = lax.axis_index('data')

    def piece(self, origin_mask, color):
        rows, cols = self.pieces[color]
        if origin_mask == 0 and self.shard is not None:
            return self.shard.at[rows, cols]
        return self.full.at[flips(self.me, origin_mask), rows, cols]

    def push(self, origin_mask, color, bit, sem_index, send_index):
        rows, cols = self.pieces[color]
        pltpu.make_async_remote_copy(
            src_ref=self.piece(origin_mask, color),
            dst_ref=self.full.at[flips(self.me, origin_mask), rows, cols],
            send_sem=self.send.at[send_index], recv_sem=self.recv.at[sem_index],
            device_id=(flip(self.me, bit),), device_id_type=MESH).start()

    def masks(self, color, stage):
        d1, d2, d3 = COLOR_ORDERS[color]
        return ((0,), (0, d1), (0, d1, d2, d1 | d2))[stage]

    def start(self, stage):
        for color in range(3):
            for mask in self.masks(color, stage):
                self.push(mask, color, COLOR_ORDERS[color][stage], 3 * color + stage, 0)

    def wait(self, stage):
        for color in range(3):
            rows, cols = self.pieces[color]
            landed = self.full.at[pl.ds(0, 2 ** stage), rows, cols]
            pltpu.make_async_copy(landed, landed, self.recv.at[3 * color + stage]).wait()

    def share(self, stage):
        for color in range(3):
            if stage < 0:
                self.push(0, color, CORE, 9, 1)
            else:
                bit = COLOR_ORDERS[color][stage]
                for mask in self.masks(color, stage):
                    self.push(mask | bit, color, CORE, 9, 1)

    def own_load(self):
        pltpu.make_async_copy(self.shard, self.own_vmem, self.own_sem).start()

    def own_store(self):
        pltpu.make_async_copy(self.shard, self.own_vmem, self.own_sem).wait()
        pltpu.make_async_copy(self.own_vmem, self.full.at[self.me], self.own_sem).start()

    def blocks(self, count, sem):
        span = self.full.at[pl.ds(0, count)]
        pltpu.make_async_copy(span, span, sem).wait()

    def shared(self, count):
        self.blocks(count, self.recv.at[9])

    def finish(self, sent, shared):
        self.blocks(sent, self.send.at[0])
        self.blocks(shared, self.send.at[1])
        if self.shard is not None:
            pltpu.make_async_copy(self.own_vmem, self.full.at[self.me], self.own_sem).wait()


GATHER_SEMS = [pltpu.SemaphoreType.DMA((10,)), pltpu.SemaphoreType.DMA((2,))]


def gather_scratch(shard):
    return GATHER_SEMS + [pltpu.VMEM(shard.shape, BF), pltpu.SemaphoreType.DMA]


def pieces_in(full):
    cols = full.shape[2]
    a = LANES * ((cols // LANES + 2) // 3)
    every = slice(None)
    return [(every, pl.ds(0, a)), (every, pl.ds(a, a)), (every, pl.ds(2 * a, cols - 2 * a))]


def pieces_out(full):
    rows = full.shape[1]
    b = 16 * (rows // 48)
    every = slice(None)
    return [(pl.ds(0, b), every), (pl.ds(b, b), every), (pl.ds(2 * b, rows - 2 * b), every)]


def gather_in(shard, full, scratch):
    recv, send, vmem, sem = scratch
    return Gather(full, pieces_in(full), (recv, send), shard, vmem, sem)


def gather_out(shard, full, scratch):
    recv, send, vmem, sem = scratch
    return Gather(full, pieces_out(full), (recv, send), shard, vmem, sem)


def full_shape(shard):
    return jax.ShapeDtypeStruct((DEVICES,) + shard.shape, BF)


def gather_kernel(with_tokens, *refs):
    if with_tokens:
        shard_in, shard_out, x_hbm, full_in, full_out, pair, *scratch = refs
        *scratch, x_vmem, x_sems = scratch
    else:
        shard_in, shard_out, full_in, full_out, *scratch = refs
    g_in, g_out = gather_in(shard_in, full_in, scratch[:4]), gather_out(shard_out, full_out, scratch[4:])
    me = lax.axis_index('data')
    greet_neighbours(*((ANTIPODE,) if with_tokens else ()))
    g_in.start(0)
    g_out.start(0)
    if with_tokens:
        trade = pltpu.make_async_remote_copy(src_ref=x_hbm, dst_ref=pair.at[1], send_sem=x_sems.at[0], recv_sem=x_sems.at[1],
                                             device_id=(flips(me, ANTIPODE),), device_id_type=MESH)
        load = pltpu.make_async_copy(x_hbm, x_vmem, x_sems.at[2])
        store = pltpu.make_async_copy(x_vmem, pair.at[0], x_sems.at[2])
        trade.start()
        load.start()
    for g in (g_in, g_out):
        g.own_load()
    for g in (g_in, g_out):
        g.share(-1)
    for g in (g_in, g_out):
        g.own_store()
    if with_tokens:
        load.wait()
        store.start()
    g_in.wait(0)
    g_in.start(1)
    g_in.share(0)
    g_out.wait(0)
    g_out.start(1)
    g_out.share(0)
    g_in.wait(1)
    g_in.start(2)
    g_in.share(1)
    g_in.wait(2)
    g_in.share(2)
    g_out.wait(1)
    g_in.shared(8)
    g_out.shared(2)
    g_in.finish(7, 8)
    g_out.finish(3, 2)
    if with_tokens:
        trade.wait()
        store.wait()


def gather_layer(shard_in, shard_out, x=None):
    with_tokens = x is not None
    out_shape = [full_shape(shard_in), full_shape(shard_out)]
    scratch = gather_scratch(shard_in) + gather_scratch(shard_out)
    args = [shard_in, shard_out]
    if with_tokens:
        args += [x]
        out_shape += [jax.ShapeDtypeStruct((2,) + x.shape, BF)]
        scratch += [pltpu.VMEM(x.shape, BF), pltpu.SemaphoreType.DMA((3,))]
    return pl.pallas_call(
        functools.partial(gather_kernel, with_tokens), out_shape=out_shape,
        in_specs=[ANY] * len(args), out_specs=[ANY] * len(out_shape), scratch_shapes=scratch,
        compiler_params=pltpu.CompilerParams(collective_id=6 if with_tokens else 0, has_side_effects=True, vmem_limit_bytes=VMEM_LIMIT),
        name='gather_with_tokens' if with_tokens else 'gather_first')(*args)


HB = 512
MT = 512


def gelu_and_slope(z):
    w = z * SQRT_HALF
    phi = 0.5 + 0.5 * lax.erf(w)
    density = jnp.exp2(LOG_DENSITY - w * w * LOG2_E)
    return z * phi, phi + z * density


def forward_kernel(last, trading, n_up, n_down, *refs):
    if not last:
        (h_ref, wi_ref, _, next_in, next_out, wo_full, a_hbm, d_ref, hn_ref, full_in, full_out,
         a_vmem, wo_vmem, a_sem, wo_sem, recv, send, *scratch) = refs
        nxt_in, nxt_out = gather_in(next_in, full_in, scratch[:4]), gather_out(next_out, full_out, scratch[4:])
    else:
        if trading:
            h_ref, wi_ref, _, y_hbm, wo_full, a_hbm, d_ref, r_ref, rb_ref, loss_ref, y_other, *scratch = refs
        else:
            h_ref, wi_ref, _, y_hbm, y_other, wo_full, a_hbm, d_ref, r_ref, rb_ref, loss_ref, *scratch = refs
        a_vmem, wo_vmem, a_sem, wo_sem, recv, send, y_vmem, late, y_sems = scratch
    w_out = Gather(wo_full, pieces_out(wo_full), (recv, send))
    step = pl.program_id(0)
    me = lax.axis_index('data')
    unit = wo_full.shape[1]
    own_blocks = n_down // 2

    def at(s, fn):
        pl.when(step == s)(fn)

    def wo_loads():
        for dev in range(DEVICES):
            yield pltpu.make_async_copy(wo_full.at[dev], wo_vmem.at[pl.ds(dev * unit, unit)], wo_sem)

    def trade_y():
        return pltpu.make_async_remote_copy(src_ref=y_hbm, dst_ref=y_other, send_sem=y_sems.at[0], recv_sem=y_sems.at[1],
                                            device_id=(flips(me, ANTIPODE),), device_id_type=MESH)

    def load_y(which):
        own = which == 0
        return pltpu.make_async_copy(y_hbm if own else y_other, y_vmem.at[which], y_sems.at[2 + which])

    def begin():
        greet_neighbours(*((ANTIPODE,) if trading else ()))
        if not last:
            nxt_in.start(0)
        w_out.start(2)
        w_out.share(1)
        if not last:
            for g in (nxt_in, nxt_out):
                g.own_load()
            for g in (nxt_in, nxt_out):
                g.share(-1)
        else:
            loss_ref[...] = jnp.zeros_like(loss_ref)
            load_y(0).start()
            if not trading:
                load_y(1).start()

    def pass_on():
        w_out.wait(2)
        w_out.share(2)
        if trading:
            trade_y().start()

    def bring_w_out():
        w_out.shared(6)
        for copy in wo_loads():
            copy.start()

    def advance_in(stage):
        nxt_in.wait(stage)
        nxt_in.start(stage + 1)
        nxt_in.share(stage)

    def advance_out():
        nxt_out.wait(0)
        nxt_out.share(0)

    at(0, begin)
    if last:
        at(n_up - 4, pass_on)
        at(n_up - 2, bring_w_out)
    else:
        def stores():
            nxt_in.own_store()
            nxt_out.own_store()

        def second():
            advance_in(0)
            nxt_out.start(0)

        def arrive_in():
            nxt_in.wait(2)
            nxt_in.share(2)
        at(1, stores)
        at(2, second)
        at(n_up - 2, pass_on)
        at(n_up - 1, functools.partial(advance_in, 1))
        at(n_up - 1, bring_w_out)
        at(n_up, advance_out)
        at(n_up + 1, lambda: nxt_out.start(1))
        at(n_up + n_down - 1, arrive_in)

    @pl.when(step < n_up)
    def _():
        base = pl.multiple_of(jnp.minimum(step, n_up - 1) * HB, HB)
        for m in range(h_ref.shape[0] // MT):
            rows = span(m, MT)
            z = jnp.dot(h_ref[rows, :], wi_ref[...], preferred_element_type=F32)
            act, slope = gelu_and_slope(z.astype(BF).astype(F32))
            a_vmem[rows, pl.ds(base, HB)] = act.astype(BF)
            d_ref[rows, :] = slope
        pltpu.make_async_copy(a_vmem.at[:, pl.ds(base, HB)], a_hbm.at[:, pl.ds(base, HB)], a_sem).start()

    def residual(h_next, which, block):
        rows = pl.ds(pl.multiple_of(block * MT, MT), MT)
        error = h_next.astype(F32) - y_vmem[which, rows, :].astype(F32)
        r = error / (own_blocks * MT)
        r_ref[...] = r
        rb_ref[...] = r.astype(BF)
        return error

    @pl.when((step >= n_up) & (step < n_up + n_down))
    def _():
        @pl.when(step == n_up)
        def _():
            pltpu.make_async_copy(wo_vmem, wo_vmem, wo_sem).wait()
            if last:
                load_y(0).wait()
                if not trading:
                    load_y(1).wait()
        block = jnp.clip(step - n_up, 0, n_down - 1)
        base = pl.multiple_of(block * MT, MT)
        branch = jnp.dot(a_vmem[pl.ds(base, MT), :], wo_vmem[...], preferred_element_type=F32)
        h_next = (h_ref[pl.ds(base, MT), :].astype(F32) + branch).astype(BF)
        if not last:
            hn_ref[...] = h_next
        else:
            if trading:
                late[pl.ds(pl.multiple_of((block % own_blocks) * MT, MT), MT), :] = h_next

            @pl.when(step < n_up + own_blocks)
            def _():
                error = residual(h_next, 0, block)
                loss_ref[...] += fold_squares(error)
            if not trading:
                @pl.when(step >= n_up + own_blocks)
                def _():
                    residual(h_next, 1, block - own_blocks)

    final = n_up + n_down - 1
    if trading:
        final += own_blocks

        @pl.when(step == n_up + n_down)
        def _():
            trade_y().wait()
            load_y(1).start()
            load_y(1).wait()

        @pl.when(step >= n_up + n_down)
        def _():
            block = jnp.clip(step - n_up - n_down, 0, own_blocks - 1)
            residual(late[pl.ds(pl.multiple_of(block * MT, MT), MT), :], 1, block)

    def end():
        pltpu.make_async_copy(a_vmem, a_hbm, a_sem).wait()
        w_out.finish(4, 6)
        if not last:
            nxt_out.wait(1)
            nxt_in.shared(8)
            nxt_out.shared(2)
            nxt_in.finish(7, 8)
            nxt_out.finish(3, 2)
    at(final, end)


def forward_layer(h, w_in_full, w_out_part, next_shards=None, y=None, y_other=None):
    tokens, width = h.shape
    hidden = w_in_full.shape[1]
    n_up, n_down = hidden // HB, tokens // MT
    last = next_shards is None
    trading = last and y_other is None
    half = n_down // 2
    up = lambda s: jnp.minimum(s, n_up - 1)
    down = lambda s: jnp.maximum(s - n_up, 0)
    if trading:
        down = lambda s: jnp.where(s < n_up + n_down, jnp.clip(s - n_up, 0, half - 1), s - n_up - half)
    row_block = pl.BlockSpec((MT, width), lambda s: (down(s), 0))
    in_specs = [pl.BlockSpec((tokens, width), lambda s: (0, 0), pipeline_mode=pl.Buffered(1)),
                pl.BlockSpec((width, HB), lambda s: (0, up(s))), ANY]
    out_specs = [ANY, ANY, pl.BlockSpec((tokens, HB), lambda s: (0, up(s)))]
    out_shape = [jax.ShapeDtypeStruct(w_out_part.shape, BF), jax.ShapeDtypeStruct((tokens, hidden), BF), jax.ShapeDtypeStruct((tokens, hidden), F32)]
    scratch = [pltpu.VMEM((tokens, hidden), BF), pltpu.VMEM((hidden, width), BF),
               pltpu.SemaphoreType.DMA, pltpu.SemaphoreType.DMA] + GATHER_SEMS
    args = [h, w_in_full, w_out_part]
    if not last:
        args += list(next_shards)
        in_specs += [ANY, ANY]
        out_specs += [row_block, ANY, ANY]
        out_shape += [jax.ShapeDtypeStruct((tokens, width), BF)] + [full_shape(sh) for sh in next_shards]
        for sh in next_shards:
            scratch += gather_scratch(sh)
    else:
        args += [y] if trading else [y, y_other]
        in_specs += [ANY] if trading else [ANY, ANY]
        out_specs += [row_block, row_block, pl.BlockSpec(SUM_TILE, lambda s: (0, 0))]
        out_shape += [jax.ShapeDtypeStruct((tokens, width), F32), jax.ShapeDtypeStruct((tokens, width), BF), jax.ShapeDtypeStruct(SUM_TILE, F32)]
        if trading:
            out_specs += [ANY]
            out_shape += [jax.ShapeDtypeStruct(y.shape, BF)]
        scratch += [pltpu.VMEM((2,) + y.shape, BF), pltpu.VMEM(y.shape, BF), pltpu.SemaphoreType.DMA((4,))]
    return pl.pallas_call(
        functools.partial(forward_kernel, last, trading, n_up, n_down), grid=(n_up + n_down + (half if trading else 0),),
        in_specs=in_specs, out_specs=out_specs, out_shape=out_shape, scratch_shapes=scratch,
        input_output_aliases={2: 0},
        compiler_params=pltpu.CompilerParams(collective_id=7 if trading else 8 if last else 1, has_side_effects=True, vmem_limit_bytes=VMEM_LIMIT),
        cost_estimate=pl.CostEstimate(flops=4 * tokens * width * hidden, bytes_accessed=70 * 2 ** 20, transcendentals=0),
        name='forward_trade' if trading else 'forward_last' if last else 'forward_gather')(*args)


NB = 512
TILE = 256
OWNERS = (1, 2, 4, 0)
TURNS = 8
TAIL = 8
LEAD = 4


def chip_at(turn):
    chip = lax.shift_right_logical(lax.axis_index('data'), 1)
    near = chip ^ (lax.shift_left(1, turn & 3) & 7)
    return jnp.where(turn < 4, near, 7 - near)


def rounded_sum(lhs_t, rhs, half):
    first = jnp.dot(lhs_t[:, :half], rhs[:half, :], preferred_element_type=F32).astype(BF).astype(F32)
    second = jnp.dot(lhs_t[:, half:], rhs[half:, :], preferred_element_type=F32).astype(BF).astype(F32)
    return first + second


def backward_kernel(with_input_grad, rb_ref, wo_ref, a_ref, d_ref, h_hbm, *refs):
    if with_input_grad:
        wi_ref, r_ref, rn_ref, rbn_ref, gi_out, go_out, *scratch = refs
    else:
        loss_ref, gi_out, go_out, loss_out, *scratch = refs
        *scratch, tiles, tile_send, tile_recv = scratch
    (rbt, ht, e_ref, gi_x, gi_send, gi_recv, go_x, go_recv,
     h_sem, dsend, drecv, gi_sent, go_sent, xrecv, own_sem, credit) = scratch
    step = pl.program_id(0)
    lead = 0 if with_input_grad else LEAD
    me = lax.axis_index('data')
    chip, core = lax.shift_right_logical(me, 1), me & 1
    tokens, width = rb_ref.shape
    half = tokens // 2
    rows_dev = ht.shape[0] // 8
    mine = 4 * rows_dev
    unit = NB // 2
    partner = (flip(me, CORE),)

    def at(s, fn):
        pl.when(step == s)(fn)

    h_base = pl.multiple_of(chip * NB, NB)

    def h_copies():
        for i in range(4):
            source = flip(chip, OWNERS[i]) if OWNERS[i] else chip
            cols = pl.multiple_of(source * 2 * rows_dev, 2 * rows_dev)
            place = pl.multiple_of(h_base + i * 2 * rows_dev, 2 * rows_dev)
            yield pltpu.make_async_copy(h_hbm.at[:, pl.ds(cols, 2 * rows_dev)], e_ref.at[:, pl.ds(place, 2 * rows_dev)], h_sem)

    def begin():
        for copy in h_copies():
            copy.start()
        if lead:
            greet_all()
            tiles[me] = loss_ref[...]
            send_to_all(tiles, tile_send, tile_recv)
        else:
            greet_neighbours()
        if lead:
            for m in range(tokens // MT):
                turn_rb(m)

    def turn_rb(m):
        rbt[:, span(m, MT)] = rb_ref[span(m, MT), :].T

    def turn_h():
        whole = e_ref.at[:, pl.ds(h_base, NB)]
        pltpu.make_async_copy(whole, whole, h_sem).wait()
        for m in range(tokens // TILE):
            cols = span(m, TILE)
            for i in range(4):
                place = pl.multiple_of(h_base + i * 2 * rows_dev, 2 * rows_dev)
                flipped = e_ref[cols, pl.ds(place, 2 * rows_dev)].T
                ht[pl.ds(pl.multiple_of(i * rows_dev + core * mine, rows_dev), rows_dev), cols] = flipped[:rows_dev]
                ht[pl.ds(pl.multiple_of(i * rows_dev + (1 - core) * mine, rows_dev), rows_dev), cols] = flipped[rows_dev:]

    def core_copy(src, dst, index):
        return pltpu.make_async_remote_copy(src_ref=src, dst_ref=dst, send_sem=dsend.at[index], recv_sem=drecv.at[index],
                                            device_id=partner, device_id_type=MESH)

    def gi_core(turn):
        return core_copy(gi_send.at[turn & 1], gi_recv.at[turn & 1], turn & 1)

    def outbox(turn):
        return 4 + (turn & 1 if lead else 0)

    def go_core(turn):
        return core_copy(go_x.at[outbox(turn)], go_recv, 2 + (outbox(turn) - 4))

    def ship(src, dst, i, sent, arrived, kept):
        if i < 3:
            pltpu.make_async_remote_copy(src_ref=src, dst_ref=dst(1 + i), send_sem=sent, recv_sem=arrived,
                                         device_id=(flip(me, 2 * OWNERS[i]),), device_id_type=MESH).start()
        else:
            pltpu.make_async_copy(src, dst(0), kept).start()

    def go_merge(turn):
        go_core(turn).wait_recv()
        go_x[turn] = go_x[turn] + go_recv[...]
        if turn < 3:
            pl.semaphore_signal(credit, inc=1, device_id=partner, device_id_type=MESH)
        ship(go_x.at[turn], lambda slot: go_out.at[slot], turn, go_sent.at[turn % 3], xrecv.at[3 + turn % 3], own_sem.at[1])

    def gi_merge(turn):
        gi_core(turn).wait_recv()
        gi_x[turn] = gi_x[turn] + gi_recv[turn & 1]
        cols = pl.ds(pl.multiple_of(chip_at(turn) * NB, NB), NB)
        for i in range(4):
            ship(gi_x.at[turn, pl.ds(i * rows_dev, rows_dev)], lambda slot: gi_out.at[slot, :, cols],
                 i, gi_sent.at[i % 3], xrecv.at[i % 3], own_sem.at[0])

    at(0, begin)
    turn = jnp.clip(step - lead, 0, TURNS - 1)
    working = (step >= lead) & (step < lead + TURNS)
    base = pl.multiple_of(chip_at(turn) * NB, NB)

    def slopes(turning):
        for m in range(tokens // MT):
            rows = span(m, MT)
            u = lax.dot_general(rb_ref[rows, :], wo_ref[...], NT, preferred_element_type=F32)
            e_ref[rows, pl.ds(base, NB)] = (d_ref[rows, :] * u).astype(BF)
            if turning:
                turn_rb(m)

    if lead:
        pl.when(working)(lambda: slopes(False))
    else:
        at(0, lambda: slopes(True))
        pl.when(working & (step > 0))(lambda: slopes(False))

    at(lead, turn_h)

    if with_input_grad:
        @pl.when(step >= TURNS)
        def _():
            start = pl.multiple_of((jnp.maximum(step - TURNS, 0) % 2) * half, half)
            for m in range(half // MT):
                rows = span(m, MT)
                u = lax.dot_general(e_ref[pl.ds(start + m * MT, MT), :], wi_ref[...], NT, preferred_element_type=F32) + r_ref[rows, :]
                rn_ref[rows, :] = u
                rbn_ref[rows, :] = u.astype(BF)

    pl.when((step >= lead + 2) & (step < lead + TURNS))(lambda: gi_core(turn).wait_send())

    @pl.when(working)
    def _():
        total = rounded_sum(ht[...], e_ref[:, pl.ds(base, NB)], half)
        gi_x[turn] = total[:mine]
        gi_send[turn & 1] = total[mine:]

    last_merge = TURNS if with_input_grad else lead + TURNS - 1
    pl.when((step >= lead + 1) & (step <= last_merge))(lambda: gi_merge(jnp.clip(step - lead - 1, 0, TURNS - 1)))

    @pl.when(working)
    def _():
        gi_core(turn).start()

    def out_grad():
        for m in range(width // MT):
            rows = span(m, MT)
            total = rounded_sum(rbt[rows, :], a_ref[...], half)
            for which in range(2):
                go_x[jnp.where(core == which, jnp.minimum(step, 3), outbox(step)), rows, :] = total[:, which * unit:(which + 1) * unit]

    pl.when((step >= 1 + bool(lead)) & (step < 4))(lambda: go_core(step).wait_send())
    pl.when(step < 4)(out_grad)
    for t in range(4):
        at(t + 1, functools.partial(go_merge, t))
    pl.when((step >= 1) & (step < 4))(lambda: pl.semaphore_wait(credit, 1))
    pl.when(step < 4)(lambda: go_core(step).start())

    def end():
        if lead:
            gi_merge(TURNS - 1)
            loss_out[...] = sum_of_all(tiles, tile_send, tile_recv)
        for t in (TURNS - 2, TURNS - 1):
            gi_core(t).wait_send()
        for t in (2, 3) if lead else (3,):
            go_core(t).wait_send()
        for kind, sent, whole in ((0, gi_sent, gi_out.at[0]), (1, go_sent, go_out.at[0])):
            pltpu.make_async_copy(whole, whole, own_sem.at[kind]).wait()
            for i in range(3):
                pltpu.make_async_copy(whole, whole, sent.at[i]).wait()
                pltpu.make_async_copy(whole, whole, xrecv.at[3 * kind + i]).wait()
    at(TURNS + (TAIL if with_input_grad else LEAD) - 1, end)


def backward_layer(rb, r, h, w_in_full, w_out_full, a, d, with_input_grad, squares):
    tokens, width = rb.shape
    hidden = a.shape[1]
    half = tokens // 2
    rows_dev = width // DEVICES
    lead = 0 if with_input_grad else LEAD
    turn = lambda s: jnp.clip(s - lead, 0, TURNS - 1)
    tail = lambda s: jnp.maximum(s - TURNS, 0)
    in_specs = [pl.BlockSpec((tokens, width), lambda s: (0, 0), pipeline_mode=pl.Buffered(1)),
                pl.BlockSpec((NB, width), lambda s: (chip_at(turn(s)), 0)),
                pl.BlockSpec((tokens, NB), lambda s: (0, chip_at(jnp.minimum(s, 3)))),
                pl.BlockSpec((tokens, NB), lambda s: (0, chip_at(turn(s)))),
                ANY]
    args = [rb, w_out_full, a, d, h]
    out_specs, out_shape = [], []
    if with_input_grad:
        block = lambda s: (tail(s) & 1, lax.shift_right_logical(tail(s), 1))
        in_specs += [pl.BlockSpec((TILE, hidden), lambda s: (lax.shift_right_logical(tail(s), 1), 0)), pl.BlockSpec((half, TILE), block)]
        args += [w_in_full, r]
        out_specs += [pl.BlockSpec((half, TILE), block)] * 2
        out_shape += [jax.ShapeDtypeStruct((tokens, width), F32), jax.ShapeDtypeStruct((tokens, width), BF)]
    else:
        in_specs += [pl.BlockSpec(SUM_TILE, lambda s: (0, 0))]
        args += [squares]
    out_specs += [ANY, ANY]
    out_shape += [jax.ShapeDtypeStruct((4, rows_dev, hidden), F32), jax.ShapeDtypeStruct((4, width, hidden // DEVICES), F32)]
    dma = pltpu.SemaphoreType.DMA
    scratch = [pltpu.VMEM((width, tokens), BF), pltpu.VMEM((8 * rows_dev, tokens), BF), pltpu.VMEM((tokens, hidden), BF),
               pltpu.VMEM((TURNS, 4 * rows_dev, NB), F32), pltpu.VMEM((2, 4 * rows_dev, NB), F32), pltpu.VMEM((2, 4 * rows_dev, NB), F32),
               pltpu.VMEM((5 + bool(lead), width, NB // 2), F32), pltpu.VMEM((width, NB // 2), F32),
               dma, dma((4,)), dma((4,)), dma((3,)), dma((3,)), dma((6,)), dma((2,)), pltpu.SemaphoreType.REGULAR]
    if not with_input_grad:
        out_specs += [pl.BlockSpec(SUM_TILE, lambda s: (0, 0))]
        out_shape += [jax.ShapeDtypeStruct(SUM_TILE, F32)]
        scratch += TILE_SCRATCH
    return pl.pallas_call(
        functools.partial(backward_kernel, with_input_grad), grid=(TURNS + (TAIL if with_input_grad else LEAD),),
        in_specs=in_specs, out_specs=out_specs, out_shape=out_shape, scratch_shapes=scratch,
        compiler_params=pltpu.CompilerParams(collective_id=2 if with_input_grad else 3, has_side_effects=True, vmem_limit_bytes=VMEM_LIMIT),
        cost_estimate=pl.CostEstimate(flops=6 * tokens * width * hidden, bytes_accessed=100 * 2 ** 20, transcendentals=0),
        name='backward' if with_input_grad else 'backward_first')(*args)


class Parts:
    def __init__(self, layers, gi, go, w_in, w_out, vgi, vgo, vw_in, vw_out, sems):
        self.layers = layers
        self.copies = []
        for l in range(layers):
            for src, dst in ((gi[l], vgi.at[l]), (go[l], vgo.at[l]), (w_in.at[l], vw_in.at[l]), (w_out.at[l], vw_out.at[l])):
                self.copies.append((l, pltpu.make_async_copy(src, dst, sems.at[len(self.copies)])))
        self.vgi, self.vgo = vgi, vgo

    def start(self):
        for l in reversed(range(self.layers)):
            for layer, copy in self.copies:
                if layer == l:
                    copy.start()

    def wait(self, l):
        for layer, copy in self.copies:
            if layer == l:
                copy.wait()

    def each(self, l, use_in, use_out, carry):
        share = 1.0 / DEVICES

        def in_rows(i, c):
            rows = pl.ds(pl.multiple_of(i * 8, 8), 8)
            total = self.vgi[l, 0, rows, :] + self.vgi[l, 1, rows, :] + self.vgi[l, 2, rows, :] + self.vgi[l, 3, rows, :]
            return use_in(rows, total * share, c)
        carry = lax.fori_loop(0, self.vgi.shape[2] // 8, in_rows, carry)

        def out_cols(i, c):
            rows = pl.ds(pl.multiple_of(i * LANES, LANES), LANES)
            total = self.vgo[l, 0, rows, :] + self.vgo[l, 1, rows, :] + self.vgo[l, 2, rows, :] + self.vgo[l, 3, rows, :]
            return use_out(rows, (total * share).T, c)
        return lax.fori_loop(0, self.vgo.shape[2] // LANES, out_cols, carry)


def fold_squares(values):
    squares = values * values
    part = jnp.sum(squares.reshape(-1, 8, squares.shape[1]), axis=0)
    return sum(part[:, i:i + LANES] for i in range(0, part.shape[1], LANES))


def perturb_kernel(layers, radius, *refs):
    gi, go = refs[:layers], refs[layers:2 * layers]
    w_in, w_out = refs[2 * layers:2 * layers + 2]
    p_in, p_out = refs[2 * layers + 2:3 * layers + 2], refs[3 * layers + 2:4 * layers + 2]
    vgi, vgo, vw_in, vw_out, g_in, g_out, sems, tiles, send, recv = refs[4 * layers + 2:]
    parts = Parts(layers, gi, go, w_in, w_out, vgi, vgo, vw_in, vw_out, sems)
    parts.start()
    greet_all()
    total = jnp.zeros(SUM_TILE, F32)
    for l in reversed(range(layers)):
        parts.wait(l)

        def use_in(rows, mean, carry, l=l):
            g_in[l, rows, :] = mean
            return carry + fold_squares(mean)

        def use_out(rows, mean, carry, l=l):
            g_out[l, :, rows] = mean
            return carry + fold_squares(mean)
        total = parts.each(l, use_in, use_out, total)
    tiles[lax.axis_index('data')] = jnp.full(SUM_TILE, jnp.sum(total), F32)
    send_to_all(tiles, send, recv)
    norm = jnp.sqrt(sum_of_all(tiles, send, recv))
    scale = (radius / norm)[0:1, 0:1]
    for l in range(layers):
        def in_rows(i, carry, l=l):
            rows = pl.ds(pl.multiple_of(i * 16, 16), 16)
            p_in[l][rows, :] = (vw_in[l, rows, :] + scale * g_in[l, rows, :]).astype(BF)
            return carry
        lax.fori_loop(0, p_in[l].shape[0] // 16, in_rows, 0)

        def out_rows(i, carry, l=l):
            rows = pl.ds(pl.multiple_of(i * 64, 64), 64)
            p_out[l][rows, :] = (vw_out[l, rows, :] + scale * g_out[l, rows, :]).astype(BF)
            return carry
        lax.fori_loop(0, p_out[l].shape[0] // 64, out_rows, 0)


def update_kernel(layers, *refs):
    gi, go = refs[:layers], refs[layers:2 * layers]
    w_in, w_out, new_in, new_out, vgi, vgo, vw_in, vw_out, sems, done = refs[2 * layers:]
    parts = Parts(layers, gi, go, w_in, w_out, vgi, vgo, vw_in, vw_out, sems)
    parts.start()
    outs = []
    for l in reversed(range(layers)):
        parts.wait(l)

        def use_in(rows, mean, carry, l=l):
            vw_in[l, rows, :] = vw_in[l, rows, :] - LEARN_RATE * mean
            return carry

        def use_out(rows, mean, carry, l=l):
            vw_out[l, :, rows] = vw_out[l, :, rows] - LEARN_RATE * mean
            return carry
        parts.each(l, use_in, use_out, 0)
        for src, dst in ((vw_in.at[l], new_in.at[l]), (vw_out.at[l], new_out.at[l])):
            outs.append(pltpu.make_async_copy(src, dst, done.at[len(outs)]))
            outs[-1].start()
    for copy in outs:
        copy.wait()


def parts_scratch(gi, go, w_in, w_out):
    layers = len(gi)
    return [pltpu.VMEM((layers,) + gi[0].shape, F32), pltpu.VMEM((layers,) + go[0].shape, F32),
            pltpu.VMEM(w_in.shape, F32), pltpu.VMEM(w_out.shape, F32)]


def perturb(gi, go, w_in, w_out, radius):
    layers = len(gi)
    outs = [jax.ShapeDtypeStruct(w_in.shape[1:], BF)] * layers + [jax.ShapeDtypeStruct(w_out.shape[1:], BF)] * layers
    res = pl.pallas_call(
        functools.partial(perturb_kernel, layers, radius), out_shape=outs,
        in_specs=[ANY] * (2 * layers + 2), out_specs=[pl.BlockSpec(memory_space=pltpu.VMEM)] * (2 * layers),
        scratch_shapes=parts_scratch(gi, go, w_in, w_out) + [
            pltpu.VMEM(w_in.shape, F32), pltpu.VMEM(w_out.shape, F32), pltpu.SemaphoreType.DMA((4 * layers,))] + TILE_SCRATCH,
        compiler_params=pltpu.CompilerParams(collective_id=4, has_side_effects=True, vmem_limit_bytes=VMEM_LIMIT),
        name='perturb')(*gi, *go, w_in, w_out)
    return res[:layers], res[layers:]


def update(gi, go, w_in, w_out):
    layers = len(gi)
    return pl.pallas_call(
        functools.partial(update_kernel, layers),
        out_shape=[jax.ShapeDtypeStruct(w_in.shape, F32), jax.ShapeDtypeStruct(w_out.shape, F32)],
        in_specs=[ANY] * (2 * layers + 2), out_specs=[ANY, ANY],
        scratch_shapes=parts_scratch(gi, go, w_in, w_out) + [
            pltpu.SemaphoreType.DMA((4 * layers,)), pltpu.SemaphoreType.DMA((2 * layers,))],
        compiler_params=pltpu.CompilerParams(vmem_limit_bytes=VMEM_LIMIT), name='update')(*gi, *go, w_in, w_out)


def sam_pass(tokens, targets, shards_in, shards_out):
    layers = len(shards_in)
    if tokens.ndim == 2:
        full_in, full_out, tokens = gather_layer(shards_in[0], shards_out[0], tokens)
    else:
        full_in, full_out = gather_layer(shards_in[0], shards_out[0])
    h_cur = tokens.reshape(-1, tokens.shape[-1])
    saved = []
    for layer in range(layers):
        w_in_full = full_in.reshape(-1, full_in.shape[-1])
        if layer + 1 < layers:
            nxt = (shards_in[layer + 1], shards_out[layer + 1])
            wo, act, slope, h_next, full_in, full_out_next = forward_layer(h_cur, w_in_full, full_out, nxt)
        else:
            wo, act, slope, r, rb, squares, *other = forward_layer(h_cur, w_in_full, full_out, None, *targets)
            if other:
                targets = (targets[0], other[0])
        saved.append((h_cur, act, slope, w_in_full, wo.reshape(-1, wo.shape[-1])))
        if layer + 1 < layers:
            h_cur, full_out = h_next, full_out_next
    g_in = [None] * layers
    g_out = [None] * layers
    for layer in reversed(range(layers)):
        h_prev, act, slope, w_in_full, w_out_full = saved[layer]
        res = backward_layer(rb, r, h_prev, w_in_full, w_out_full, act, slope, layer > 0, squares)
        if layer > 0:
            r, rb, g_in[layer], g_out[layer] = res
        else:
            g_in[layer], g_out[layer], squares = res
    return squares, g_in, g_out, tokens, targets


def solution(mesh):
    groups = mesh.shape['data']

    def device_step(x_blk, y_blk, w_in_sh, w_out_sh):
        layers = w_in_sh.shape[0]
        model_dim = w_out_sh.shape[2]
        radius = RHO_FRAC * math.sqrt(layers * model_dim)
        x_tok = x_blk.reshape(-1, model_dim)
        y_tok = y_blk.reshape(-1, model_dim)
        span = range(layers)
        _, g_in, g_out, x_pair, y_pair = sam_pass(x_tok, (y_tok,), [w_in_sh[l].astype(BF) for l in span], [w_out_sh[l].astype(BF) for l in span])
        pert_in, pert_out = perturb(g_in, g_out, w_in_sh, w_out_sh, radius)
        squares, gp_in, gp_out, _, _ = sam_pass(x_pair, y_pair, pert_in, pert_out)
        mean_loss = jnp.sum(squares) * (0.5 / (x_tok.shape[0] * groups))
        new_in, new_out = update(gp_in, gp_out, w_in_sh, w_out_sh)
        return new_in, new_out, mean_loss

    return jax.shard_map(device_step, mesh=mesh,
                         in_specs=(P('data', None, None), P('data', None, None), P(None, 'data', None), P(None, 'data', None)),
                         out_specs=(P(None, 'data', None), P(None, 'data', None), P()),
                         check_vma=False)
```

```python
import functools
import math
import jax
import jax.numpy as jnp
from jax import lax
from jax.experimental import pallas as pl
from jax.experimental.pallas import tpu as pltpu
from jax.sharding import PartitionSpec as P

RHO_FRAC = 0.1
LEARN_RATE = 0.5
BF = jnp.bfloat16
F32 = jnp.float32
MESH = pl.DeviceIdType.MESH
DEVICES = 16
LANES = 128
SUM_TILE = (8, LANES)
SQRT_HALF = math.sqrt(0.5)
LOG2_E = math.log2(math.e)
LOG_DENSITY = -0.5 * math.log2(2.0 * math.pi)
VMEM_LIMIT = 63 * 2 ** 20
NT = (((1,), (1,)), ((), ()))
CORE, AX_X, AX_Y, AX_Z = 1, 2, 4, 8
ANTIPODE = AX_X | AX_Y | AX_Z
COLOR_ORDERS = ((AX_X, AX_Y, AX_Z), (AX_Y, AX_Z, AX_X), (AX_Z, AX_X, AX_Y))
ANY = pl.BlockSpec(memory_space=pl.ANY)


def origin(step):
    return 0, 0


def span(index, size):
    return pl.ds(index * size, size)


def flip(dev, bit):
    return dev ^ bit


def flips(dev, mask):
    return dev ^ mask


def greet_neighbours(*more):
    me = lax.axis_index('data')
    barrier = pltpu.get_barrier_semaphore()
    masks = (CORE, AX_X, AX_Y, AX_Z) + more
    for mask in masks:
        pl.semaphore_signal(barrier, inc=1, device_id=(flips(me, mask),), device_id_type=MESH)
    pl.semaphore_wait(barrier, len(masks))


def greet_all():
    me = lax.axis_index('data')
    barrier = pltpu.get_barrier_semaphore()
    for other in range(1, DEVICES):
        pl.semaphore_signal(barrier, inc=1, device_id=((me + other) % DEVICES,), device_id_type=MESH)


def send_to_all(tiles, send, recv):
    me = lax.axis_index('data')
    pl.semaphore_wait(pltpu.get_barrier_semaphore(), DEVICES - 1)
    for other in range(1, DEVICES):
        pltpu.make_async_remote_copy(src_ref=tiles.at[me], dst_ref=tiles.at[me], send_sem=send, recv_sem=recv,
                                     device_id=((me + other) % DEVICES,), device_id_type=MESH).start()


def sum_of_all(tiles, send, recv):
    others = tiles.at[pl.ds(0, DEVICES - 1)]
    pltpu.make_async_copy(others, others, recv).wait()
    pltpu.make_async_copy(others, others, send).wait()
    return jnp.sum(tiles[...], axis=0)


TILE_SCRATCH = [pltpu.VMEM((DEVICES,) + SUM_TILE, F32), pltpu.SemaphoreType.DMA, pltpu.SemaphoreType.DMA]


class Gather:
    def __init__(self, full, pieces, sems, shard=None, own_vmem=None, own_sem=None):
        self.shard, self.full, self.pieces = shard, full, pieces
        self.recv, self.send = sems
        self.own_vmem, self.own_sem = own_vmem, own_sem
        self.me = lax.axis_index('data')

    def piece(self, origin_mask, color):
        rows, cols = self.pieces[color]
        if origin_mask == 0 and self.shard is not None:
            return self.shard.at[rows, cols]
        return self.full.at[flips(self.me, origin_mask), rows, cols]

    def push(self, origin_mask, color, bit, sem_index, send_index):
        rows, cols = self.pieces[color]
        pltpu.make_async_remote_copy(
            src_ref=self.piece(origin_mask, color),
            dst_ref=self.full.at[flips(self.me, origin_mask), rows, cols],
            send_sem=self.send.at[send_index], recv_sem=self.recv.at[sem_index],
            device_id=(flip(self.me, bit),), device_id_type=MESH).start()

    def masks(self, color, stage):
        d1, d2, d3 = COLOR_ORDERS[color]
        return ((0,), (0, d1), (0, d1, d2, d1 | d2))[stage]

    def start(self, stage):
        for color in range(3):
            for mask in self.masks(color, stage):
                self.push(mask, color, COLOR_ORDERS[color][stage], 3 * color + stage, 0)

    def wait(self, stage):
        for color in range(3):
            rows, cols = self.pieces[color]
            landed = self.full.at[pl.ds(0, 2 ** stage), rows, cols]
            pltpu.make_async_copy(landed, landed, self.recv.at[3 * color + stage]).wait()

    def share(self, stage):
        for color in range(3):
            if stage < 0:
                self.push(0, color, CORE, 9, 1)
            else:
                bit = COLOR_ORDERS[color][stage]
                for mask in self.masks(color, stage):
                    self.push(mask | bit, color, CORE, 9, 1)

    def own_load(self):
        pltpu.make_async_copy(self.shard, self.own_vmem, self.own_sem).start()

    def own_store(self):
        pltpu.make_async_copy(self.shard, self.own_vmem, self.own_sem).wait()
        pltpu.make_async_copy(self.own_vmem, self.full.at[self.me], self.own_sem).start()

    def blocks(self, count, sem):
        span = self.full.at[pl.ds(0, count)]
        pltpu.make_async_copy(span, span, sem).wait()

    def shared(self, count):
        self.blocks(count, self.recv.at[9])

    def finish(self, sent, shared):
        self.blocks(sent, self.send.at[0])
        self.blocks(shared, self.send.at[1])
        if self.shard is not None:
            pltpu.make_async_copy(self.own_vmem, self.full.at[self.me], self.own_sem).wait()


GATHER_SEMS = [pltpu.SemaphoreType.DMA((10,)), pltpu.SemaphoreType.DMA((2,))]


def gather_scratch(shard):
    return GATHER_SEMS + [pltpu.VMEM(shard.shape, BF), pltpu.SemaphoreType.DMA]


def pieces_in(full):
    cols = full.shape[2]
    a = LANES * ((cols // LANES + 2) // 3)
    every = slice(None)
    return [(every, pl.ds(0, a)), (every, pl.ds(a, a)), (every, pl.ds(2 * a, cols - 2 * a))]


def pieces_out(full):
    rows = full.shape[1]
    b = 16 * (rows // 48)
    every = slice(None)
    return [(pl.ds(0, b), every), (pl.ds(b, b), every), (pl.ds(2 * b, rows - 2 * b), every)]


def gather_in(shard, full, scratch):
    recv, send, vmem, sem = scratch
    return Gather(full, pieces_in(full), (recv, send), shard, vmem, sem)


def gather_out(shard, full, scratch):
    recv, send, vmem, sem = scratch
    return Gather(full, pieces_out(full), (recv, send), shard, vmem, sem)


def full_shape(shard):
    return jax.ShapeDtypeStruct((DEVICES,) + shard.shape, BF)


def gather_kernel(with_tokens, *refs):
    if with_tokens:
        shard_in, shard_out, x_hbm, full_in, full_out, pair, *scratch = refs
        *scratch, x_vmem, x_sems = scratch
    else:
        shard_in, shard_out, full_in, full_out, *scratch = refs
    g_in, g_out = gather_in(shard_in, full_in, scratch[:4]), gather_out(shard_out, full_out, scratch[4:])
    me = lax.axis_index('data')
    greet_neighbours(*((ANTIPODE,) if with_tokens else ()))
    g_in.start(0)
    g_out.start(0)
    if with_tokens:
        trade = pltpu.make_async_remote_copy(src_ref=x_hbm, dst_ref=pair.at[1], send_sem=x_sems.at[0], recv_sem=x_sems.at[1],
                                             device_id=(flips(me, ANTIPODE),), device_id_type=MESH)
        load = pltpu.make_async_copy(x_hbm, x_vmem, x_sems.at[2])
        store = pltpu.make_async_copy(x_vmem, pair.at[0], x_sems.at[2])
        trade.start()
        load.start()
    for g in (g_in, g_out):
        g.own_load()
    for g in (g_in, g_out):
        g.share(-1)
    for g in (g_in, g_out):
        g.own_store()
    if with_tokens:
        load.wait()
        store.start()
    g_in.wait(0)
    g_in.start(1)
    g_in.share(0)
    g_out.wait(0)
    g_out.start(1)
    g_out.share(0)
    g_in.wait(1)
    g_in.start(2)
    g_in.share(1)
    g_in.wait(2)
    g_in.share(2)
    g_out.wait(1)
    g_in.shared(8)
    g_out.shared(2)
    g_in.finish(7, 8)
    g_out.finish(3, 2)
    if with_tokens:
        trade.wait()
        store.wait()


def gather_layer(shard_in, shard_out, x=None):
    with_tokens = x is not None
    out_shape = [full_shape(shard_in), full_shape(shard_out)]
    scratch = gather_scratch(shard_in) + gather_scratch(shard_out)
    args = [shard_in, shard_out]
    if with_tokens:
        args += [x]
        out_shape += [jax.ShapeDtypeStruct((2,) + x.shape, BF)]
        scratch += [pltpu.VMEM(x.shape, BF), pltpu.SemaphoreType.DMA((3,))]
    return pl.pallas_call(
        functools.partial(gather_kernel, with_tokens), out_shape=out_shape,
        in_specs=[ANY] * len(args), out_specs=[ANY] * len(out_shape), scratch_shapes=scratch,
        compiler_params=pltpu.CompilerParams(collective_id=6 if with_tokens else 0, has_side_effects=True, vmem_limit_bytes=VMEM_LIMIT),
        name='gather_with_tokens' if with_tokens else 'gather_first')(*args)


HB = 512
MT = 512


def gelu_and_slope(z):
    w = z * SQRT_HALF
    phi = 0.5 + 0.5 * lax.erf(w)
    density = jnp.exp2(LOG_DENSITY - w * w * LOG2_E)
    return z * phi, phi + z * density


def forward_kernel(last, trading, n_up, n_down, *refs):
    if not last:
        (h_ref, wi_ref, _, next_in, next_out, wo_full, a_hbm, d_ref, hn_ref, full_in, full_out,
         a_vmem, wo_vmem, a_sem, wo_sem, recv, send, *scratch) = refs
        nxt_in, nxt_out = gather_in(next_in, full_in, scratch[:4]), gather_out(next_out, full_out, scratch[4:])
    else:
        if trading:
            h_ref, wi_ref, _, y_hbm, wo_full, a_hbm, d_ref, r_ref, rb_ref, loss_ref, y_other, *scratch = refs
        else:
            h_ref, wi_ref, _, y_hbm, y_other, wo_full, a_hbm, d_ref, r_ref, rb_ref, loss_ref, *scratch = refs
        a_vmem, wo_vmem, a_sem, wo_sem, recv, send, y_vmem, late, y_sems = scratch
    w_out = Gather(wo_full, pieces_out(wo_full), (recv, send))
    step = pl.program_id(0)
    me = lax.axis_index('data')
    unit = wo_full.shape[1]
    own_blocks = n_down // 2

    def at(s, fn):
        pl.when(step == s)(fn)

    def wo_loads():
        for dev in range(DEVICES):
            yield pltpu.make_async_copy(wo_full.at[dev], wo_vmem.at[pl.ds(dev * unit, unit)], wo_sem)

    def trade_y():
        return pltpu.make_async_remote_copy(src_ref=y_hbm, dst_ref=y_other, send_sem=y_sems.at[0], recv_sem=y_sems.at[1],
                                            device_id=(flips(me, ANTIPODE),), device_id_type=MESH)

    def load_y(which):
        own = which == 0
        return pltpu.make_async_copy(y_hbm if own else y_other, y_vmem.at[which], y_sems.at[2 + which])

    def begin():
        greet_neighbours(*((ANTIPODE,) if trading else ()))
        if not last:
            nxt_in.start(0)
        w_out.start(2)
        w_out.share(1)
        if not last:
            for g in (nxt_in, nxt_out):
                g.own_load()
            for g in (nxt_in, nxt_out):
                g.share(-1)
        else:
            loss_ref[...] = jnp.zeros_like(loss_ref)
            load_y(0).start()
            if not trading:
                load_y(1).start()

    def pass_on():
        w_out.wait(2)
        w_out.share(2)
        if trading:
            trade_y().start()

    def bring_w_out():
        w_out.shared(6)
        for copy in wo_loads():
            copy.start()

    def advance_in(stage):
        nxt_in.wait(stage)
        nxt_in.start(stage + 1)
        nxt_in.share(stage)

    def advance_out():
        nxt_out.wait(0)
        nxt_out.share(0)

    at(0, begin)
    if last:
        at(n_up - 4, pass_on)
        at(n_up - 2, bring_w_out)
    else:
        def stores():
            nxt_in.own_store()
            nxt_out.own_store()

        def second():
            advance_in(0)
            nxt_out.start(0)

        def arrive_in():
            nxt_in.wait(2)
            nxt_in.share(2)
        at(1, stores)
        at(2, second)
        at(n_up - 2, pass_on)
        at(n_up - 1, functools.partial(advance_in, 1))
        at(n_up - 1, bring_w_out)
        at(n_up, advance_out)
        at(n_up + 1, lambda: nxt_out.start(1))
        at(n_up + n_down - 1, arrive_in)

    @pl.when(step < n_up)
    def _():
        base = pl.multiple_of(jnp.minimum(step, n_up - 1) * HB, HB)
        for m in range(h_ref.shape[0] // MT):
            rows = span(m, MT)
            z = jnp.dot(h_ref[rows, :], wi_ref[...], preferred_element_type=F32)
            act, slope = gelu_and_slope(z.astype(BF).astype(F32))
            a_vmem[rows, pl.ds(base, HB)] = act.astype(BF)
            d_ref[rows, :] = slope
        pltpu.make_async_copy(a_vmem.at[:, pl.ds(base, HB)], a_hbm.at[:, pl.ds(base, HB)], a_sem).start()

    def residual(h_next, which, block):
        rows = pl.ds(pl.multiple_of(block * MT, MT), MT)
        error = h_next.astype(F32) - y_vmem[which, rows, :].astype(F32)
        r = error / (own_blocks * MT)
        r_ref[...] = r
        rb_ref[...] = r.astype(BF)
        return error

    @pl.when((step >= n_up) & (step < n_up + n_down))
    def _():
        @pl.when(step == n_up)
        def _():
            pltpu.make_async_copy(wo_vmem, wo_vmem, wo_sem).wait()
            if last:
                load_y(0).wait()
                if not trading:
                    load_y(1).wait()
        block = jnp.clip(step - n_up, 0, n_down - 1)
        base = pl.multiple_of(block * MT, MT)
        branch = jnp.dot(a_vmem[pl.ds(base, MT), :], wo_vmem[...], preferred_element_type=F32)
        h_next = (h_ref[pl.ds(base, MT), :].astype(F32) + branch).astype(BF)
        if not last:
            hn_ref[...] = h_next
        else:
            if trading:
                late[pl.ds(pl.multiple_of((block % own_blocks) * MT, MT), MT), :] = h_next

            @pl.when(step < n_up + own_blocks)
            def _():
                error = residual(h_next, 0, block)
                loss_ref[...] += fold_squares(error)
            if not trading:
                @pl.when(step >= n_up + own_blocks)
                def _():
                    residual(h_next, 1, block - own_blocks)

    final = n_up + n_down - 1
    if trading:
        final += own_blocks

        @pl.when(step == n_up + n_down)
        def _():
            trade_y().wait()
            load_y(1).start()
            load_y(1).wait()

        @pl.when(step >= n_up + n_down)
        def _():
            block = jnp.clip(step - n_up - n_down, 0, own_blocks - 1)
            residual(late[pl.ds(pl.multiple_of(block * MT, MT), MT), :], 1, block)

    def end():
        pltpu.make_async_copy(a_vmem, a_hbm, a_sem).wait()
        w_out.finish(4, 6)
        if not last:
            nxt_out.wait(1)
            nxt_in.shared(8)
            nxt_out.shared(2)
            nxt_in.finish(7, 8)
            nxt_out.finish(3, 2)
    at(final, end)


def forward_layer(h, w_in_full, w_out_part, next_shards=None, y=None, y_other=None):
    tokens, width = h.shape
    hidden = w_in_full.shape[1]
    n_up, n_down = hidden // HB, tokens // MT
    last = next_shards is None
    trading = last and y_other is None
    half = n_down // 2
    up = lambda s: jnp.minimum(s, n_up - 1)
    down = lambda s: jnp.maximum(s - n_up, 0)
    if trading:
        down = lambda s: jnp.where(s < n_up + n_down, jnp.clip(s - n_up, 0, half - 1), s - n_up - half)
    row_block = pl.BlockSpec((MT, width), lambda s: (down(s), 0))
    in_specs = [pl.BlockSpec((tokens, width), origin, pipeline_mode=pl.Buffered(1)),
                pl.BlockSpec((width, HB), lambda s: (0, up(s))), ANY]
    out_specs = [ANY, ANY, pl.BlockSpec((tokens, HB), lambda s: (0, up(s)))]
    out_shape = [jax.ShapeDtypeStruct(w_out_part.shape, BF), jax.ShapeDtypeStruct((tokens, hidden), BF), jax.ShapeDtypeStruct((tokens, hidden), F32)]
    scratch = [pltpu.VMEM((tokens, hidden), BF), pltpu.VMEM((hidden, width), BF),
               pltpu.SemaphoreType.DMA, pltpu.SemaphoreType.DMA] + GATHER_SEMS
    args = [h, w_in_full, w_out_part]
    if not last:
        args += list(next_shards)
        in_specs += [ANY, ANY]
        out_specs += [row_block, ANY, ANY]
        out_shape += [jax.ShapeDtypeStruct((tokens, width), BF)] + [full_shape(sh) for sh in next_shards]
        for sh in next_shards:
            scratch += gather_scratch(sh)
    else:
        args += [y] if trading else [y, y_other]
        in_specs += [ANY] if trading else [ANY, ANY]
        out_specs += [row_block, row_block, pl.BlockSpec(SUM_TILE, origin)]
        out_shape += [jax.ShapeDtypeStruct((tokens, width), F32), jax.ShapeDtypeStruct((tokens, width), BF), jax.ShapeDtypeStruct(SUM_TILE, F32)]
        if trading:
            out_specs += [ANY]
            out_shape += [jax.ShapeDtypeStruct(y.shape, BF)]
        scratch += [pltpu.VMEM((2,) + y.shape, BF), pltpu.VMEM(y.shape, BF), pltpu.SemaphoreType.DMA((4,))]
    return pl.pallas_call(
        functools.partial(forward_kernel, last, trading, n_up, n_down), grid=(n_up + n_down + (half if trading else 0),),
        in_specs=in_specs, out_specs=out_specs, out_shape=out_shape, scratch_shapes=scratch,
        input_output_aliases={2: 0},
        compiler_params=pltpu.CompilerParams(collective_id=7 if trading else 8 if last else 1, has_side_effects=True, vmem_limit_bytes=VMEM_LIMIT),
        cost_estimate=pl.CostEstimate(flops=4 * tokens * width * hidden, bytes_accessed=70 * 2 ** 20, transcendentals=0),
        name='forward_trade' if trading else 'forward_last' if last else 'forward_gather')(*args)


NB = 512
TILE = 256
OWNERS = (1, 2, 4, 0)
TURNS = 8
TAIL = 8
LEAD = 8


def chip_at(turn):
    chip = lax.shift_right_logical(lax.axis_index('data'), 1)
    near = chip ^ (lax.shift_left(1, turn & 3) & 7)
    return jnp.where(turn < 4, near, 7 - near)


def rounded_sum(lhs_t, rhs, half):
    first = jnp.dot(lhs_t[:, :half], rhs[:half, :], preferred_element_type=F32).astype(BF).astype(F32)
    second = jnp.dot(lhs_t[:, half:], rhs[half:, :], preferred_element_type=F32).astype(BF).astype(F32)
    return first + second


def backward_kernel(with_input_grad, rb_ref, wo_hbm, a_hbm, d_hbm, h_hbm, *refs):
    if with_input_grad:
        wi_hbm, r_hbm, rn_ref, rbn_ref, gi_out, go_out, *scratch = refs
        *scratch, wi_buf, r_buf, wi_sem, r_sem = scratch
    else:
        loss_ref, gi_out, go_out, loss_out, *scratch = refs
        *scratch, tiles, tile_send, tile_recv = scratch
    (rbt, ht, e_ref, wo_buf, a_buf, d_buf, gi_x, gi_send, gi_recv, go_x, go_send, go_recv,
     h_sem, wo_sem, a_sem, d_sem, gi_dsend, gi_drecv, go_dsend, go_drecv, gi_sent, go_sent, xrecv, own_sem) = scratch
    step = pl.program_id(0)
    lead = 0 if with_input_grad else LEAD
    me = lax.axis_index('data')
    chip, core = lax.shift_right_logical(me, 1), me & 1
    tokens, width = rb_ref.shape
    half = tokens // 2
    rows_dev = ht.shape[0] // 8
    mine = 4 * rows_dev
    unit = NB // 2
    partner = (flip(me, CORE),)
    a_slots = a_buf.shape[0]

    def at(s, fn):
        pl.when(step == s)(fn)

    def hidden_cols(turn):
        return pl.ds(pl.multiple_of(chip_at(turn) * NB, NB), NB)

    def wo_copy(turn):
        return pltpu.make_async_copy(wo_hbm.at[hidden_cols(turn)], wo_buf.at[turn & 1], wo_sem.at[turn & 1])

    def d_copy(turn):
        return pltpu.make_async_copy(d_hbm.at[:, hidden_cols(turn)], d_buf.at[turn & 1], d_sem.at[turn & 1])

    def a_copy(owner):
        slot = owner & (a_slots - 1)
        return pltpu.make_async_copy(a_hbm.at[:, hidden_cols(owner)], a_buf.at[slot], a_sem.at[slot])

    def wi_copy(block):
        rows = pl.ds(pl.multiple_of(block * TILE, TILE), TILE)
        return pltpu.make_async_copy(wi_hbm.at[rows], wi_buf.at[block & 1], wi_sem.at[block & 1])

    def r_copy(index):
        rows = pl.ds(pl.multiple_of((index & 1) * half, half), half)
        cols = pl.ds(pl.multiple_of(lax.shift_right_logical(index, 1) * TILE, TILE), TILE)
        return pltpu.make_async_copy(r_hbm.at[rows, cols], r_buf.at[index & 1], r_sem.at[index & 1])

    h_base = pl.multiple_of(chip * NB, NB)

    def h_copies():
        for i in range(4):
            source = flip(chip, OWNERS[i]) if OWNERS[i] else chip
            cols = pl.multiple_of(source * 2 * rows_dev, 2 * rows_dev)
            place = pl.multiple_of(h_base + i * 2 * rows_dev, 2 * rows_dev)
            yield pltpu.make_async_copy(h_hbm.at[:, pl.ds(cols, 2 * rows_dev)], e_ref.at[:, pl.ds(place, 2 * rows_dev)], h_sem)

    def begin():
        first = jnp.int32(0)
        pair = (first, first + 1)
        owners = tuple(first + i for i in range(a_slots))
        starts = [(wo_copy, pair), (d_copy, pair), (a_copy, owners)]
        for copy, indices in starts[::-1] if lead else starts:
            for i in indices:
                copy(i).start()
        for copy in h_copies():
            copy.start()
        if lead:
            greet_all()
            tiles[me] = loss_ref[...]
            send_to_all(tiles, tile_send, tile_recv)
            for m in range(tokens // MT):
                turn_rb(m)
        else:
            greet_neighbours()

    def turn_rb(m):
        rbt[:, span(m, MT)] = rb_ref[span(m, MT), :].T

    def turn_h():
        whole = e_ref.at[:, pl.ds(h_base, NB)]
        pltpu.make_async_copy(whole, whole, h_sem).wait()
        for m in range(tokens // TILE):
            cols = span(m, TILE)
            for i in range(4):
                place = pl.multiple_of(h_base + i * 2 * rows_dev, 2 * rows_dev)
                flipped = e_ref[cols, pl.ds(place, 2 * rows_dev)].T
                ht[pl.ds(pl.multiple_of(i * rows_dev + core * mine, rows_dev), rows_dev), cols] = flipped[:rows_dev]
                ht[pl.ds(pl.multiple_of(i * rows_dev + (1 - core) * mine, rows_dev), rows_dev), cols] = flipped[rows_dev:]

    def core_copy(src, dst, send, recv):
        return pltpu.make_async_remote_copy(src_ref=src, dst_ref=dst, send_sem=send, recv_sem=recv, device_id=partner, device_id_type=MESH)

    def gi_core(turn):
        slot = turn & 1
        return core_copy(gi_send.at[slot], gi_recv.at[slot], gi_dsend.at[slot], gi_drecv.at[slot])

    def outbox(piece):
        return piece & (go_send.shape[0] - 1)

    def go_core(piece):
        out, slot = outbox(piece), piece & 3
        return core_copy(go_send.at[out], go_recv.at[slot], go_dsend.at[out], go_drecv.at[slot])

    def ship(src, dst, i, sent, arrived, kept):
        if i < 3:
            pltpu.make_async_remote_copy(src_ref=src, dst_ref=dst(1 + i), send_sem=sent, recv_sem=arrived,
                                         device_id=(flip(me, 2 * OWNERS[i]),), device_id_type=MESH).start()
        else:
            pltpu.make_async_copy(src, dst(0), kept).start()

    def go_merge(piece):
        owner, part = piece & 3, piece >> 2
        rows = span(part, MT)
        go_core(piece).wait_recv()
        go_x[owner, rows, :] = go_x[owner, rows, :] + go_recv[piece & 3]
        ship(go_x.at[owner, rows], lambda slot: go_out.at[slot, rows], owner, go_sent.at[owner % 3], xrecv.at[3 + owner % 3], own_sem.at[1])

    def out_grad(owner, part, piece):
        rows = pl.ds(pl.multiple_of(part * MT, MT), MT)
        total = rounded_sum(rbt[rows, :], a_buf[owner & (a_slots - 1)], half)

        @pl.when(core == 0)
        def _():
            go_x[owner, rows, :] = total[:, :unit]
            go_send[outbox(piece)] = total[:, unit:]

        @pl.when(core == 1)
        def _():
            go_x[owner, rows, :] = total[:, unit:]
            go_send[outbox(piece)] = total[:, :unit]

    def gi_merge(turn):
        gi_core(turn).wait_recv()
        gi_x[turn] = gi_x[turn] + gi_recv[turn & 1]
        cols = hidden_cols(turn)
        for i in range(4):
            ship(gi_x.at[turn, pl.ds(i * rows_dev, rows_dev)], lambda slot: gi_out.at[slot, :, cols],
                 i, gi_sent.at[i % 3], xrecv.at[i % 3], own_sem.at[0])

    at(0, begin)
    turn = jnp.clip(step - lead, 0, TURNS - 1)
    working = (step >= lead) & (step < lead + TURNS)
    base = pl.multiple_of(chip_at(turn) * NB, NB)

    if lead:
        @pl.when(step < lead)
        def _():
            piece = jnp.minimum(step, 7)
            owner = piece & 3
            pl.when(piece < 4)(lambda: a_copy(owner).wait())
            pl.when(piece >= 4)(lambda: go_core(piece).wait_send())
            out_grad(owner, lax.shift_right_logical(piece, 2), piece)
        for p in range(8):
            at(p + 2, functools.partial(go_merge, p))
        pl.when(step < lead)(lambda: go_core(step).start())

    @pl.when(working)
    def _():
        @pl.when((step > lead) & (turn < TURNS - 1))
        def _():
            wo_copy(turn + 1).start()
            d_copy(turn + 1).start()
        wo_copy(turn).wait()
        d_copy(turn).wait()

    def slopes(turning):
        slot = turn & 1
        for m in range(tokens // MT):
            rows = span(m, MT)
            u = lax.dot_general(rb_ref[rows, :], wo_buf[slot], NT, preferred_element_type=F32)
            e_ref[rows, pl.ds(base, NB)] = (d_buf[slot, rows, :] * u).astype(BF)
            if turning:
                turn_rb(m)

    if lead:
        pl.when(working)(lambda: slopes(False))
    else:
        at(0, lambda: slopes(True))
        pl.when(working & (step > 0))(lambda: slopes(False))

    at(lead, turn_h)

    if with_input_grad:
        def ahead():
            for i in range(2):
                wi_copy(jnp.int32(i)).start()
                r_copy(jnp.int32(i)).start()
        at(TURNS - 2, ahead)

        @pl.when(step >= TURNS)
        def _():
            index = jnp.maximum(step - TURNS, 0)
            block = lax.shift_right_logical(index, 1)
            side = index & 1

            @pl.when((index > 0) & (index < TAIL - 1))
            def _():
                r_copy(index + 1).start()

            @pl.when((side == 0) & (index > 0) & (index < TAIL - 2))
            def _():
                wi_copy(block + 1).start()
            pl.when(side == 0)(lambda: wi_copy(block).wait())
            r_copy(index).wait()
            for m in range(half // MT):
                rows = span(m, MT)
                left = e_ref[pl.ds(pl.multiple_of(side * half + m * MT, MT), MT), :]
                u = lax.dot_general(left, wi_buf[block & 1], NT, preferred_element_type=F32) + r_buf[side, rows, :]
                rn_ref[rows, :] = u
                rbn_ref[rows, :] = u.astype(BF)

    pl.when((step >= lead + 2) & (step < lead + TURNS))(lambda: gi_core(turn).wait_send())

    @pl.when(working)
    def _():
        total = rounded_sum(ht[...], e_ref[:, pl.ds(base, NB)], half)
        gi_x[turn] = total[:mine]
        gi_send[turn & 1] = total[mine:]

    last_merge = TURNS if with_input_grad else lead + TURNS - 1
    pl.when((step >= lead + 1) & (step <= last_merge))(lambda: gi_merge(jnp.clip(step - lead - 1, 0, TURNS - 1)))

    @pl.when(working)
    def _():
        gi_core(turn).start()

    if not lead:
        @pl.when(step < 4)
        def _():
            for i in range(2):
                piece = 2 * jnp.minimum(step, 3) + i
                owner = piece & 3
                a_copy(owner).wait()
                pl.when(step >= 1)(lambda: go_core(piece).wait_send())
                out_grad(owner, lax.shift_right_logical(piece, 2), piece)
                pl.when(step < 3)(lambda: a_copy((owner + 2) & 3).start())
        for p in range(8):
            at((p >> 1) + 1, functools.partial(go_merge, p))

        @pl.when(step < 4)
        def _():
            for part in range(2):
                go_core(2 * jnp.minimum(step, 3) + part).start()

    def end():
        if lead:
            gi_merge(TURNS - 1)
            loss_out[...] = sum_of_all(tiles, tile_send, tile_recv)
        for t in (TURNS - 2, TURNS - 1):
            gi_core(t).wait_send()
        for piece in range(go_send.shape[0]):
            go_core(piece).wait_send()
        for kind, sent, whole in ((0, gi_sent, gi_out.at[0]), (1, go_sent, go_out.at[0])):
            pltpu.make_async_copy(whole, whole, own_sem.at[kind]).wait()
            for i in range(3):
                pltpu.make_async_copy(whole, whole, sent.at[i]).wait()
                pltpu.make_async_copy(whole, whole, xrecv.at[3 * kind + i]).wait()
    at(TURNS + (TAIL if with_input_grad else LEAD) - 1, end)


def backward_layer(rb, r, h, w_in_full, w_out_full, a, d, with_input_grad, squares):
    tokens, width = rb.shape
    hidden = a.shape[1]
    half = tokens // 2
    rows_dev = width // DEVICES
    tail = lambda s: jnp.maximum(s - TURNS, 0)
    in_specs = [pl.BlockSpec((tokens, width), origin, pipeline_mode=pl.Buffered(1))] + [ANY] * 4
    args = [rb, w_out_full, a, d, h]
    out_specs, out_shape = [], []
    dma = pltpu.SemaphoreType.DMA
    two, three, four = dma((2,)), dma((3,)), dma((4,))
    small = (4 * rows_dev, NB)
    piece = (MT, NB // 2)
    scratch = [pltpu.VMEM((width, tokens), BF), pltpu.VMEM((8 * rows_dev, tokens), BF), pltpu.VMEM((tokens, hidden), BF),
               pltpu.VMEM((2, NB, width), BF), pltpu.VMEM((2 if with_input_grad else 4, tokens, NB), BF), pltpu.VMEM((2, tokens, NB), F32),
               pltpu.VMEM((TURNS,) + small, F32), pltpu.VMEM((2,) + small, F32), pltpu.VMEM((2,) + small, F32),
               pltpu.VMEM((4, width, NB // 2), F32), pltpu.VMEM((2 if with_input_grad else 4,) + piece, F32), pltpu.VMEM((4,) + piece, F32),
               dma, two, four, two, two, two, four, four, three, three, dma((6,)), two]
    if with_input_grad:
        block = lambda s: (tail(s) & 1, lax.shift_right_logical(tail(s), 1))
        in_specs += [ANY, ANY]
        args += [w_in_full, r]
        out_specs += [pl.BlockSpec((half, TILE), block)] * 2
        out_shape += [jax.ShapeDtypeStruct((tokens, width), F32), jax.ShapeDtypeStruct((tokens, width), BF)]
        scratch += [pltpu.VMEM((2, TILE, hidden), BF), pltpu.VMEM((2, half, TILE), F32), two, two]
    else:
        in_specs += [pl.BlockSpec(SUM_TILE, origin)]
        args += [squares]
        scratch += TILE_SCRATCH
    out_specs += [ANY, ANY]
    out_shape += [jax.ShapeDtypeStruct((4, rows_dev, hidden), F32), jax.ShapeDtypeStruct((4, width, hidden // DEVICES), F32)]
    if not with_input_grad:
        out_specs += [pl.BlockSpec(SUM_TILE, origin)]
        out_shape += [jax.ShapeDtypeStruct(SUM_TILE, F32)]
    return pl.pallas_call(
        functools.partial(backward_kernel, with_input_grad), grid=(TURNS + (TAIL if with_input_grad else LEAD),),
        in_specs=in_specs, out_specs=out_specs, out_shape=out_shape, scratch_shapes=scratch,
        compiler_params=pltpu.CompilerParams(collective_id=2 if with_input_grad else 3, has_side_effects=True, vmem_limit_bytes=VMEM_LIMIT),
        cost_estimate=pl.CostEstimate(flops=6 * tokens * width * hidden, bytes_accessed=100 * 2 ** 20, transcendentals=0),
        name='backward' if with_input_grad else 'backward_first')(*args)


class Parts:
    def __init__(self, layers, gi, go, w_in, w_out, vgi, vgo, vw_in, vw_out, sems):
        self.layers = layers
        self.copies = []
        for l in range(layers):
            for src, dst in ((gi[l], vgi.at[l]), (go[l], vgo.at[l]), (w_in.at[l], vw_in.at[l]), (w_out.at[l], vw_out.at[l])):
                self.copies.append((l, pltpu.make_async_copy(src, dst, sems.at[len(self.copies)])))
        self.vgi, self.vgo = vgi, vgo

    def start(self):
        for l in reversed(range(self.layers)):
            for layer, copy in self.copies:
                if layer == l:
                    copy.start()

    def wait(self, l):
        for layer, copy in self.copies:
            if layer == l:
                copy.wait()

    def each(self, l, use_in, use_out, carry):
        share = 1.0 / DEVICES

        def in_rows(i, c):
            rows = pl.ds(pl.multiple_of(i * 8, 8), 8)
            total = self.vgi[l, 0, rows, :] + self.vgi[l, 1, rows, :] + self.vgi[l, 2, rows, :] + self.vgi[l, 3, rows, :]
            return use_in(rows, total * share, c)
        carry = lax.fori_loop(0, self.vgi.shape[2] // 8, in_rows, carry)

        def out_cols(i, c):
            rows = pl.ds(pl.multiple_of(i * LANES, LANES), LANES)
            total = self.vgo[l, 0, rows, :] + self.vgo[l, 1, rows, :] + self.vgo[l, 2, rows, :] + self.vgo[l, 3, rows, :]
            return use_out(rows, (total * share).T, c)
        return lax.fori_loop(0, self.vgo.shape[2] // LANES, out_cols, carry)


def fold_squares(values):
    squares = values * values
    part = jnp.sum(squares.reshape(-1, 8, squares.shape[1]), axis=0)
    return sum(part[:, i:i + LANES] for i in range(0, part.shape[1], LANES))


def perturb_kernel(layers, radius, *refs):
    gi, go = refs[:layers], refs[layers:2 * layers]
    w_in, w_out = refs[2 * layers:2 * layers + 2]
    p_in, p_out = refs[2 * layers + 2:3 * layers + 2], refs[3 * layers + 2:4 * layers + 2]
    vgi, vgo, vw_in, vw_out, g_in, g_out, sems, tiles, send, recv = refs[4 * layers + 2:]
    parts = Parts(layers, gi, go, w_in, w_out, vgi, vgo, vw_in, vw_out, sems)
    parts.start()
    greet_all()
    total = jnp.zeros(SUM_TILE, F32)
    for l in reversed(range(layers)):
        parts.wait(l)

        def use_in(rows, mean, carry, l=l):
            g_in[l, rows, :] = mean
            return carry + fold_squares(mean)

        def use_out(rows, mean, carry, l=l):
            g_out[l, :, rows] = mean
            return carry + fold_squares(mean)
        total = parts.each(l, use_in, use_out, total)
    tiles[lax.axis_index('data')] = jnp.full(SUM_TILE, jnp.sum(total), F32)
    send_to_all(tiles, send, recv)
    norm = jnp.sqrt(sum_of_all(tiles, send, recv))
    scale = (radius / norm)[0:1, 0:1]
    for l in range(layers):
        def in_rows(i, carry, l=l):
            rows = pl.ds(pl.multiple_of(i * 16, 16), 16)
            p_in[l][rows, :] = (vw_in[l, rows, :] + scale * g_in[l, rows, :]).astype(BF)
            return carry
        lax.fori_loop(0, p_in[l].shape[0] // 16, in_rows, 0)

        def out_rows(i, carry, l=l):
            rows = pl.ds(pl.multiple_of(i * 64, 64), 64)
            p_out[l][rows, :] = (vw_out[l, rows, :] + scale * g_out[l, rows, :]).astype(BF)
            return carry
        lax.fori_loop(0, p_out[l].shape[0] // 64, out_rows, 0)


def update_kernel(layers, *refs):
    gi, go = refs[:layers], refs[layers:2 * layers]
    w_in, w_out, new_in, new_out, vgi, vgo, vw_in, vw_out, sems, done = refs[2 * layers:]
    parts = Parts(layers, gi, go, w_in, w_out, vgi, vgo, vw_in, vw_out, sems)
    parts.start()
    outs = []
    for l in reversed(range(layers)):
        parts.wait(l)

        def use_in(rows, mean, carry, l=l):
            vw_in[l, rows, :] = vw_in[l, rows, :] - LEARN_RATE * mean
            return carry

        def use_out(rows, mean, carry, l=l):
            vw_out[l, :, rows] = vw_out[l, :, rows] - LEARN_RATE * mean
            return carry
        parts.each(l, use_in, use_out, 0)
        for src, dst in ((vw_in.at[l], new_in.at[l]), (vw_out.at[l], new_out.at[l])):
            outs.append(pltpu.make_async_copy(src, dst, done.at[len(outs)]))
            outs[-1].start()
    for copy in outs:
        copy.wait()


def parts_scratch(gi, go, w_in, w_out):
    layers = len(gi)
    return [pltpu.VMEM((layers,) + gi[0].shape, F32), pltpu.VMEM((layers,) + go[0].shape, F32),
            pltpu.VMEM(w_in.shape, F32), pltpu.VMEM(w_out.shape, F32)]


def perturb(gi, go, w_in, w_out, radius):
    layers = len(gi)
    outs = [jax.ShapeDtypeStruct(w_in.shape[1:], BF)] * layers + [jax.ShapeDtypeStruct(w_out.shape[1:], BF)] * layers
    res = pl.pallas_call(
        functools.partial(perturb_kernel, layers, radius), out_shape=outs,
        in_specs=[ANY] * (2 * layers + 2), out_specs=[pl.BlockSpec(memory_space=pltpu.VMEM)] * (2 * layers),
        scratch_shapes=parts_scratch(gi, go, w_in, w_out) + [
            pltpu.VMEM(w_in.shape, F32), pltpu.VMEM(w_out.shape, F32), pltpu.SemaphoreType.DMA((4 * layers,))] + TILE_SCRATCH,
        compiler_params=pltpu.CompilerParams(collective_id=4, has_side_effects=True, vmem_limit_bytes=VMEM_LIMIT),
        name='perturb')(*gi, *go, w_in, w_out)
    return res[:layers], res[layers:]


def update(gi, go, w_in, w_out):
    layers = len(gi)
    return pl.pallas_call(
        functools.partial(update_kernel, layers),
        out_shape=[jax.ShapeDtypeStruct(w_in.shape, F32), jax.ShapeDtypeStruct(w_out.shape, F32)],
        in_specs=[ANY] * (2 * layers + 2), out_specs=[ANY, ANY],
        scratch_shapes=parts_scratch(gi, go, w_in, w_out) + [
            pltpu.SemaphoreType.DMA((4 * layers,)), pltpu.SemaphoreType.DMA((2 * layers,))],
        compiler_params=pltpu.CompilerParams(vmem_limit_bytes=VMEM_LIMIT), name='update')(*gi, *go, w_in, w_out)


def sam_pass(tokens, targets, shards_in, shards_out):
    layers = len(shards_in)
    if tokens.ndim == 2:
        full_in, full_out, tokens = gather_layer(shards_in[0], shards_out[0], tokens)
    else:
        full_in, full_out = gather_layer(shards_in[0], shards_out[0])
    h_cur = tokens.reshape(-1, tokens.shape[-1])
    saved = []
    for layer in range(layers):
        w_in_full = full_in.reshape(-1, full_in.shape[-1])
        if layer + 1 < layers:
            nxt = (shards_in[layer + 1], shards_out[layer + 1])
            wo, act, slope, h_next, full_in, full_out_next = forward_layer(h_cur, w_in_full, full_out, nxt)
        else:
            wo, act, slope, r, rb, squares, *other = forward_layer(h_cur, w_in_full, full_out, None, *targets)
            if other:
                targets = (targets[0], other[0])
        saved.append((h_cur, act, slope, w_in_full, wo.reshape(-1, wo.shape[-1])))
        if layer + 1 < layers:
            h_cur, full_out = h_next, full_out_next
    g_in = [None] * layers
    g_out = [None] * layers
    for layer in reversed(range(layers)):
        h_prev, act, slope, w_in_full, w_out_full = saved[layer]
        res = backward_layer(rb, r, h_prev, w_in_full, w_out_full, act, slope, layer > 0, squares)
        if layer > 0:
            r, rb, g_in[layer], g_out[layer] = res
        else:
            g_in[layer], g_out[layer], squares = res
    return squares, g_in, g_out, tokens, targets


def solution(mesh):
    groups = mesh.shape['data']

    def device_step(x_blk, y_blk, w_in_sh, w_out_sh):
        layers = w_in_sh.shape[0]
        model_dim = w_out_sh.shape[2]
        radius = RHO_FRAC * math.sqrt(layers * model_dim)
        x_tok = x_blk.reshape(-1, model_dim)
        y_tok = y_blk.reshape(-1, model_dim)
        span = range(layers)
        _, g_in, g_out, x_pair, y_pair = sam_pass(x_tok, (y_tok,), [w_in_sh[l].astype(BF) for l in span], [w_out_sh[l].astype(BF) for l in span])
        pert_in, pert_out = perturb(g_in, g_out, w_in_sh, w_out_sh, radius)
        squares, gp_in, gp_out, _, _ = sam_pass(x_pair, y_pair, pert_in, pert_out)
        mean_loss = jnp.sum(squares) * (0.5 / (x_tok.shape[0] * groups))
        new_in, new_out = update(gp_in, gp_out, w_in_sh, w_out_sh)
        return new_in, new_out, mean_loss

    return jax.shard_map(device_step, mesh=mesh,
                         in_specs=(P('data', None, None), P('data', None, None), P(None, 'data', None), P(None, 'data', None)),
                         out_specs=(P(None, 'data', None), P(None, 'data', None), P()),
                         check_vma=False)
```

```python
import functools
import math
import jax
import jax.numpy as jnp
from jax import lax
from jax.experimental import pallas as pl
from jax.experimental.pallas import tpu as pltpu
from jax.sharding import PartitionSpec as P

RHO_FRAC = 0.1
LEARN_RATE = 0.5
BF = jnp.bfloat16
F32 = jnp.float32
MESH = pl.DeviceIdType.MESH
DEVICES = 16
LANES = 128
SUM_TILE = (8, LANES)
SQRT_HALF = math.sqrt(0.5)
LOG2_E = math.log2(math.e)
LOG_DENSITY = -0.5 * math.log2(2.0 * math.pi)
VMEM_LIMIT = 63 * 2 ** 20
NT = (((1,), (1,)), ((), ()))
CORE, AX_X, AX_Y, AX_Z = 1, 2, 4, 8
ANTIPODE = AX_X | AX_Y | AX_Z
COLOR_ORDERS = ((AX_X, AX_Y, AX_Z), (AX_Y, AX_Z, AX_X), (AX_Z, AX_X, AX_Y))
ANY = pl.BlockSpec(memory_space=pl.ANY)


def origin(step):
    return 0, 0


def span(index, size):
    return pl.ds(index * size, size)


def aligned(index, size):
    return pl.ds(pl.multiple_of(index * size, size), size)


def halve(index):
    return lax.shift_right_logical(index, 1)


def parity(index):
    return index & 1


def flip(dev, bit):
    return dev ^ bit


def flips(dev, mask):
    return dev ^ mask


def greet_neighbours(*more):
    me = lax.axis_index('data')
    barrier = pltpu.get_barrier_semaphore()
    masks = (CORE, AX_X, AX_Y, AX_Z) + more
    for mask in masks:
        pl.semaphore_signal(barrier, inc=1, device_id=(flips(me, mask),), device_id_type=MESH)
    pl.semaphore_wait(barrier, len(masks))


def greet_all():
    me = lax.axis_index('data')
    barrier = pltpu.get_barrier_semaphore()
    for other in range(1, DEVICES):
        pl.semaphore_signal(barrier, inc=1, device_id=((me + other) % DEVICES,), device_id_type=MESH)


def send_to_all(tiles, send, recv):
    me = lax.axis_index('data')
    pl.semaphore_wait(pltpu.get_barrier_semaphore(), DEVICES - 1)
    for other in range(1, DEVICES):
        pltpu.make_async_remote_copy(src_ref=tiles.at[me], dst_ref=tiles.at[me], send_sem=send, recv_sem=recv,
                                     device_id=((me + other) % DEVICES,), device_id_type=MESH).start()


def sum_of_all(tiles, send, recv):
    others = tiles.at[pl.ds(0, DEVICES - 1)]
    pltpu.make_async_copy(others, others, recv).wait()
    pltpu.make_async_copy(others, others, send).wait()
    return jnp.sum(tiles[...], axis=0)


TILE_SCRATCH = [pltpu.VMEM((DEVICES,) + SUM_TILE, F32), pltpu.SemaphoreType.DMA, pltpu.SemaphoreType.DMA]


class Gather:
    def __init__(self, full, pieces, sems, shard=None, own_vmem=None, own_sem=None):
        self.shard, self.full, self.pieces = shard, full, pieces
        self.recv, self.send = sems
        self.own_vmem, self.own_sem = own_vmem, own_sem
        self.me = lax.axis_index('data')

    def piece(self, origin_mask, color):
        rows, cols = self.pieces[color]
        if origin_mask == 0 and self.shard is not None:
            return self.shard.at[rows, cols]
        return self.full.at[flips(self.me, origin_mask), rows, cols]

    def push(self, origin_mask, color, bit, sem_index, send_index):
        rows, cols = self.pieces[color]
        pltpu.make_async_remote_copy(
            src_ref=self.piece(origin_mask, color),
            dst_ref=self.full.at[flips(self.me, origin_mask), rows, cols],
            send_sem=self.send.at[send_index], recv_sem=self.recv.at[sem_index],
            device_id=(flip(self.me, bit),), device_id_type=MESH).start()

    def masks(self, color, stage):
        d1, d2, d3 = COLOR_ORDERS[color]
        return ((0,), (0, d1), (0, d1, d2, d1 | d2))[stage]

    def start(self, stage):
        for color in range(3):
            for mask in self.masks(color, stage):
                self.push(mask, color, COLOR_ORDERS[color][stage], 3 * color + stage, 0)

    def wait(self, stage):
        for color in range(3):
            rows, cols = self.pieces[color]
            landed = self.full.at[pl.ds(0, 2 ** stage), rows, cols]
            pltpu.make_async_copy(landed, landed, self.recv.at[3 * color + stage]).wait()

    def share(self, stage):
        for color in range(3):
            if stage < 0:
                self.push(0, color, CORE, 9, 1)
            else:
                bit = COLOR_ORDERS[color][stage]
                for mask in self.masks(color, stage):
                    self.push(mask | bit, color, CORE, 9, 1)

    def own_load(self):
        pltpu.make_async_copy(self.shard, self.own_vmem, self.own_sem).start()

    def own_store(self, in_vmem=False):
        if in_vmem:
            self.own_vmem = self.shard
        else:
            pltpu.make_async_copy(self.shard, self.own_vmem, self.own_sem).wait()
        pltpu.make_async_copy(self.own_vmem, self.full.at[self.me], self.own_sem).start()

    def blocks(self, count, sem):
        span = self.full.at[pl.ds(0, count)]
        pltpu.make_async_copy(span, span, sem).wait()

    def shared(self, count):
        self.blocks(count, self.recv.at[9])

    def finish(self, sent, shared):
        self.blocks(sent, self.send.at[0])
        self.blocks(shared, self.send.at[1])
        if self.shard is not None:
            pltpu.make_async_copy(self.own_vmem, self.full.at[self.me], self.own_sem).wait()


GATHER_SEMS = [pltpu.SemaphoreType.DMA((10,)), pltpu.SemaphoreType.DMA((2,))]


def gather_scratch(shard):
    return GATHER_SEMS + [pltpu.VMEM(shard.shape, BF), pltpu.SemaphoreType.DMA]


def pieces_in(full):
    cols = full.shape[2]
    a = LANES * ((cols // LANES + 2) // 3)
    every = slice(None)
    return [(every, pl.ds(0, a)), (every, pl.ds(a, a)), (every, pl.ds(2 * a, cols - 2 * a))]


def pieces_out(full):
    rows = full.shape[1]
    b = 16 * (rows // 48)
    every = slice(None)
    return [(pl.ds(0, b), every), (pl.ds(b, b), every), (pl.ds(2 * b, rows - 2 * b), every)]


def gather_in(shard, full, scratch):
    recv, send, vmem, sem = scratch
    return Gather(full, pieces_in(full), (recv, send), shard, vmem, sem)


def gather_out(shard, full, scratch):
    recv, send, vmem, sem = scratch
    return Gather(full, pieces_out(full), (recv, send), shard, vmem, sem)


def full_shape(shard):
    return jax.ShapeDtypeStruct((DEVICES,) + shard.shape, BF)


def gather_kernel(with_tokens, *refs):
    me = lax.axis_index('data')
    if with_tokens:
        masters, (x_hbm, full_in, full_out, pair), refs = refs[:2], refs[2:6], refs[6:]
        layers = masters[0].shape[0]
        casts, refs = (refs[:layers], refs[layers:2 * layers]), refs[2 * layers:]
        scratch, (x_vmem, x_sems), wide, narrow, (load_sems, cast_sems) = refs[:8], refs[8:10], refs[10:12], refs[12:14], refs[14:]
        loads = [[pltpu.make_async_copy(masters[k].at[l], wide[k].at[l], load_sems.at[k, l]) for l in range(layers)] for k in range(2)]
        stores = [pltpu.make_async_copy(narrow[k].at[l], casts[k][l], cast_sems.at[k, l]) for l in range(layers) for k in range(2)]
        for l in range(layers):
            for k in range(2):
                loads[k][l].start()

        def cast(l):
            for k in range(2):
                loads[k][l].wait()
                narrow[k][l] = wide[k][l].astype(BF)
        cast(0)
        shard_in, shard_out = narrow[0].at[0], narrow[1].at[0]
    else:
        shard_in, shard_out, full_in, full_out, *scratch = refs
    g_in, g_out = gather_in(shard_in, full_in, scratch[:4]), gather_out(shard_out, full_out, scratch[4:])
    greet_neighbours(*((ANTIPODE,) if with_tokens else ()))
    g_in.start(0)
    g_out.start(0)
    if with_tokens:
        trade = pltpu.make_async_remote_copy(src_ref=x_hbm, dst_ref=pair.at[1], send_sem=x_sems.at[0], recv_sem=x_sems.at[1],
                                             device_id=(flips(me, ANTIPODE),), device_id_type=MESH)
        load = pltpu.make_async_copy(x_hbm, x_vmem, x_sems.at[2])
        store = pltpu.make_async_copy(x_vmem, pair.at[0], x_sems.at[2])
        trade.start()
        load.start()
    both = (g_in, g_out)
    if not with_tokens:
        for g in both:
            g.own_load()
    for g in both:
        g.share(-1)
    for g in both:
        g.own_store(with_tokens)
    if with_tokens:
        load.wait()
        store.start()
        for l in range(1, layers):
            cast(l)
        for copy in stores:
            copy.start()
    g_in.wait(0)
    g_in.start(1)
    g_in.share(0)
    g_out.wait(0)
    g_out.start(1)
    g_out.share(0)
    g_in.wait(1)
    g_in.start(2)
    g_in.share(1)
    g_in.wait(2)
    g_in.share(2)
    g_out.wait(1)
    g_in.shared(8)
    g_out.shared(2)
    g_in.finish(7, 8)
    g_out.finish(3, 2)
    if with_tokens:
        trade.wait()
        store.wait()
        for copy in stores:
            copy.wait()


def gather_layer(shard_in, shard_out, x=None):
    with_tokens = x is not None
    args = [shard_in, shard_out]
    dma = pltpu.SemaphoreType.DMA
    if with_tokens:
        layers = shard_in.shape[0]
        rows = [jax.ShapeDtypeStruct(sh.shape[1:], BF) for sh in args]
        out_shape = [full_shape(sh) for sh in rows] + [jax.ShapeDtypeStruct((2,) + x.shape, BF)] + rows[:1] * layers + rows[1:] * layers
        scratch = sum((gather_scratch(sh) for sh in rows), []) + [pltpu.VMEM(x.shape, BF), dma((3,))]
        scratch += [pltpu.VMEM(sh.shape, kind) for kind in (F32, BF) for sh in args] + [dma((2, layers))] * 2
        args += [x]
    else:
        out_shape = [full_shape(sh) for sh in args]
        scratch = sum((gather_scratch(sh) for sh in args), [])
    return pl.pallas_call(
        functools.partial(gather_kernel, with_tokens), out_shape=out_shape,
        in_specs=[ANY] * len(args), out_specs=[ANY] * len(out_shape), scratch_shapes=scratch,
        compiler_params=pltpu.CompilerParams(collective_id=6 if with_tokens else 0, has_side_effects=True, vmem_limit_bytes=VMEM_LIMIT),
        name='gather_with_tokens' if with_tokens else 'gather_first')(*args)


HB = 512
MT = 512


def gelu_and_slope(z):
    w = z * SQRT_HALF
    phi = 0.5 + 0.5 * lax.erf(w)
    density = jnp.exp2(LOG_DENSITY - w * w * LOG2_E)
    return z * phi, phi + z * density


def forward_kernel(last, trading, n_up, n_down, *refs):
    if not last:
        (h_hbm, wi_ref, _, next_in, next_out, wo_full, a_hbm, d_ref, hn_ref, full_in, full_out,
         h_ref, a_vmem, wo_vmem, h_sem, a_sem, wo_sem, recv, send, *scratch) = refs
        nxt_in, nxt_out = gather_in(next_in, full_in, scratch[:4]), gather_out(next_out, full_out, scratch[4:])
    else:
        if trading:
            h_hbm, wi_ref, _, y_hbm, wo_full, a_hbm, d_ref, r_ref, rb_ref, loss_ref, y_other, *scratch = refs
        else:
            h_hbm, wi_ref, _, y_hbm, y_other, wo_full, a_hbm, d_ref, r_ref, rb_ref, loss_ref, *scratch = refs
        h_ref, a_vmem, wo_vmem, h_sem, a_sem, wo_sem, recv, send, y_vmem, late, y_sems = scratch
    w_out = Gather(wo_full, pieces_out(wo_full), (recv, send))
    step = pl.program_id(0)
    me = lax.axis_index('data')
    unit = wo_full.shape[1]
    own_blocks = n_down // 2

    def at(s, fn):
        pl.when(step == s)(fn)

    def wo_loads():
        for dev in range(DEVICES):
            yield pltpu.make_async_copy(wo_full.at[dev], wo_vmem.at[pl.ds(dev * unit, unit)], wo_sem)

    def trade_y():
        return pltpu.make_async_remote_copy(src_ref=y_hbm, dst_ref=y_other, send_sem=y_sems.at[0], recv_sem=y_sems.at[1],
                                            device_id=(flips(me, ANTIPODE),), device_id_type=MESH)

    def load_y(which):
        own = which == 0
        return pltpu.make_async_copy(y_hbm if own else y_other, y_vmem.at[which], y_sems.at[2 + which])

    def begin():
        h_load = pltpu.make_async_copy(h_hbm, h_ref, h_sem)
        h_load.start()
        greet_neighbours(*((ANTIPODE,) if trading else ()))
        if not last:
            nxt_in.start(0)
        w_out.start(2)
        w_out.share(1)
        if not last:
            for g in (nxt_in, nxt_out):
                g.own_load()
            for g in (nxt_in, nxt_out):
                g.share(-1)
        else:
            loss_ref[...] = jnp.zeros_like(loss_ref)
            load_y(0).start()
            if not trading:
                load_y(1).start()
        h_load.wait()

    def pass_on():
        w_out.wait(2)
        w_out.share(2)
        if trading:
            trade_y().start()

    def bring_w_out():
        w_out.shared(6)
        for copy in wo_loads():
            copy.start()

    def advance_in(stage):
        nxt_in.wait(stage)
        nxt_in.start(stage + 1)
        nxt_in.share(stage)

    def advance_out():
        nxt_out.wait(0)
        nxt_out.share(0)

    at(0, begin)
    if last:
        at(n_up - 4, pass_on)
        at(n_up - 2, bring_w_out)
    else:
        def stores():
            nxt_in.own_store()
            nxt_out.own_store()

        def second():
            advance_in(0)
            nxt_out.start(0)

        def arrive_in():
            nxt_in.wait(2)
            nxt_in.share(2)
        at(1, stores)
        at(2, second)
        at(n_up - 2, pass_on)
        at(n_up - 1, functools.partial(advance_in, 1))
        at(n_up - 1, bring_w_out)
        at(n_up, advance_out)
        at(n_up + 1, lambda: nxt_out.start(1))
        at(n_up + n_down - 1, arrive_in)

    @pl.when(step < n_up)
    def _():
        base = pl.multiple_of(jnp.minimum(step, n_up - 1) * HB, HB)
        for m in range(h_ref.shape[0] // MT):
            rows = span(m, MT)
            z = jnp.dot(h_ref[rows, :], wi_ref[...], preferred_element_type=F32)
            act, slope = gelu_and_slope(z.astype(BF).astype(F32))
            a_vmem[rows, pl.ds(base, HB)] = act.astype(BF)
            d_ref[rows, :] = slope
        pltpu.make_async_copy(a_vmem.at[:, pl.ds(base, HB)], a_hbm.at[:, pl.ds(base, HB)], a_sem).start()

    def residual(h_next, which, block):
        rows = aligned(block, MT)
        error = h_next.astype(F32) - y_vmem[which, rows, :].astype(F32)
        r = error / (own_blocks * MT)
        r_ref[...] = r
        rb_ref[...] = r.astype(BF)
        return error

    @pl.when((step >= n_up) & (step < n_up + n_down))
    def _():
        @pl.when(step == n_up)
        def _():
            pltpu.make_async_copy(wo_vmem, wo_vmem, wo_sem).wait()
            if last:
                load_y(0).wait()
                if not trading:
                    load_y(1).wait()
        block = jnp.clip(step - n_up, 0, n_down - 1)
        base = pl.multiple_of(block * MT, MT)
        branch = jnp.dot(a_vmem[pl.ds(base, MT), :], wo_vmem[...], preferred_element_type=F32)
        h_next = (h_ref[pl.ds(base, MT), :].astype(F32) + branch).astype(BF)
        if not last:
            hn_ref[...] = h_next
        else:
            if trading:
                late[aligned((block % own_blocks), MT), :] = h_next

            @pl.when(step < n_up + own_blocks)
            def _():
                error = residual(h_next, 0, block)
                loss_ref[...] += fold_squares(error)
            if not trading:
                @pl.when(step >= n_up + own_blocks)
                def _():
                    residual(h_next, 1, block - own_blocks)

    final = n_up + n_down - 1
    if trading:
        final += own_blocks

        @pl.when(step == n_up + n_down)
        def _():
            trade_y().wait()
            load_y(1).start()
            load_y(1).wait()

        @pl.when(step >= n_up + n_down)
        def _():
            block = jnp.clip(step - n_up - n_down, 0, own_blocks - 1)
            residual(late[aligned(block, MT), :], 1, block)

    def end():
        pltpu.make_async_copy(a_vmem, a_hbm, a_sem).wait()
        w_out.finish(4, 6)
        if not last:
            nxt_out.wait(1)
            nxt_in.shared(8)
            nxt_out.shared(2)
            nxt_in.finish(7, 8)
            nxt_out.finish(3, 2)
    at(final, end)


def forward_layer(h, w_in_full, w_out_part, next_shards=None, y=None, y_other=None):
    tokens, width = h.shape
    hidden = w_in_full.shape[1]
    n_up, n_down = hidden // HB, tokens // MT
    last = next_shards is None
    trading = last and y_other is None
    half = n_down // 2
    up = lambda s: jnp.minimum(s, n_up - 1)
    down = lambda s: jnp.maximum(s - n_up, 0)
    if trading:
        down = lambda s: jnp.where(s < n_up + n_down, jnp.clip(s - n_up, 0, half - 1), s - n_up - half)
    row_block = pl.BlockSpec((MT, width), lambda s: (down(s), 0))
    in_specs = [ANY, pl.BlockSpec((width, HB), lambda s: (0, up(s))), ANY]
    out_specs = [ANY, ANY, pl.BlockSpec((tokens, HB), lambda s: (0, up(s)))]
    out_shape = [jax.ShapeDtypeStruct(w_out_part.shape, BF), jax.ShapeDtypeStruct((tokens, hidden), BF), jax.ShapeDtypeStruct((tokens, hidden), F32)]
    scratch = [pltpu.VMEM((tokens, width), BF), pltpu.VMEM((tokens, hidden), BF), pltpu.VMEM((hidden, width), BF),
               pltpu.SemaphoreType.DMA, pltpu.SemaphoreType.DMA, pltpu.SemaphoreType.DMA] + GATHER_SEMS
    args = [h, w_in_full, w_out_part]
    if not last:
        args += list(next_shards)
        in_specs += [ANY, ANY]
        out_specs += [row_block, ANY, ANY]
        out_shape += [jax.ShapeDtypeStruct((tokens, width), BF)] + [full_shape(sh) for sh in next_shards]
        for sh in next_shards:
            scratch += gather_scratch(sh)
    else:
        args += [y] if trading else [y, y_other]
        in_specs += [ANY] if trading else [ANY, ANY]
        out_specs += [row_block, row_block, pl.BlockSpec(SUM_TILE, origin)]
        out_shape += [jax.ShapeDtypeStruct((tokens, width), F32), jax.ShapeDtypeStruct((tokens, width), BF), jax.ShapeDtypeStruct(SUM_TILE, F32)]
        if trading:
            out_specs += [ANY]
            out_shape += [jax.ShapeDtypeStruct(y.shape, BF)]
        scratch += [pltpu.VMEM((2,) + y.shape, BF), pltpu.VMEM(y.shape, BF), pltpu.SemaphoreType.DMA((4,))]
    return pl.pallas_call(
        functools.partial(forward_kernel, last, trading, n_up, n_down), grid=(n_up + n_down + (half if trading else 0),),
        in_specs=in_specs, out_specs=out_specs, out_shape=out_shape, scratch_shapes=scratch,
        input_output_aliases={2: 0},
        compiler_params=pltpu.CompilerParams(collective_id=7 if trading else 8 if last else 1, has_side_effects=True, vmem_limit_bytes=VMEM_LIMIT),
        cost_estimate=pl.CostEstimate(flops=4 * tokens * width * hidden, bytes_accessed=70 * 2 ** 20, transcendentals=0),
        name='forward_trade' if trading else 'forward_last' if last else 'forward_gather')(*args)


NB = 512
TILE = 256
OWNERS = (1, 2, 4, 0)
TURNS = 8
TAIL = 8
LEAD = 8


def chip_at(turn):
    chip = halve(lax.axis_index('data'))
    near = chip ^ (lax.shift_left(1, turn & 3) & 7)
    return jnp.where(turn < 4, near, 7 - near)


def rounded_sum(lhs_t, rhs, half):
    first = jnp.dot(lhs_t[:, :half], rhs[:half, :], preferred_element_type=F32).astype(BF).astype(F32)
    second = jnp.dot(lhs_t[:, half:], rhs[half:, :], preferred_element_type=F32).astype(BF).astype(F32)
    return first + second


def backward_kernel(with_input_grad, rb_ref, wo_hbm, a_hbm, d_hbm, h_hbm, *refs):
    if with_input_grad:
        wi_hbm, r_hbm, rn_ref, rbn_ref, gi_out, go_out, *scratch = refs
        *scratch, wi_buf, r_buf, wi_sem, r_sem = scratch
    else:
        loss_ref, gi_out, go_out, loss_out, *scratch = refs
        *scratch, tiles, tile_send, tile_recv = scratch
    (rbt, ht, e_ref, wo_buf, a_buf, d_buf, gi_x, gi_send, gi_recv, go_x, go_send, go_recv,
     h_sem, wo_sem, a_sem, d_sem, gi_dsend, gi_drecv, go_dsend, go_drecv, gi_sent, go_sent, xrecv, own_sem) = scratch
    step = pl.program_id(0)
    lead = 0 if with_input_grad else LEAD
    me = lax.axis_index('data')
    chip, core = halve(me), parity(me)
    tokens, width = rb_ref.shape
    half = tokens // 2
    rows_dev = ht.shape[0] // 8
    mine = 4 * rows_dev
    unit = NB // 2
    partner = (flip(me, CORE),)
    a_slots = a_buf.shape[0]

    def at(s, fn):
        pl.when(step == s)(fn)

    def hidden_cols(turn):
        return aligned(chip_at(turn), NB)

    def wo_copy(turn):
        return pltpu.make_async_copy(wo_hbm.at[hidden_cols(turn)], wo_buf.at[parity(turn)], wo_sem.at[parity(turn)])

    def d_copy(turn):
        return pltpu.make_async_copy(d_hbm.at[:, hidden_cols(turn)], d_buf.at[parity(turn)], d_sem.at[parity(turn)])

    def a_copy(owner):
        slot = owner & (a_slots - 1)
        return pltpu.make_async_copy(a_hbm.at[:, hidden_cols(owner)], a_buf.at[slot], a_sem.at[slot])

    def wi_copy(block):
        rows = aligned(block, TILE)
        return pltpu.make_async_copy(wi_hbm.at[rows], wi_buf.at[parity(block)], wi_sem.at[parity(block)])

    def r_copy(index):
        rows = aligned(parity(index), half)
        cols = aligned(halve(index), TILE)
        return pltpu.make_async_copy(r_hbm.at[rows, cols], r_buf.at[parity(index)], r_sem.at[parity(index)])

    h_base = pl.multiple_of(chip * NB, NB)

    def h_copies():
        for i in range(4):
            source = flip(chip, OWNERS[i]) if OWNERS[i] else chip
            cols = pl.multiple_of(source * 2 * rows_dev, 2 * rows_dev)
            place = pl.multiple_of(h_base + i * 2 * rows_dev, 2 * rows_dev)
            yield pltpu.make_async_copy(h_hbm.at[:, pl.ds(cols, 2 * rows_dev)], e_ref.at[:, pl.ds(place, 2 * rows_dev)], h_sem)

    def begin():
        first = jnp.int32(0)
        pair = (first, first + 1)
        owners = tuple(first + i for i in range(a_slots))
        starts = [(wo_copy, pair), (d_copy, pair), (a_copy, owners)]
        for copy, indices in starts[::-1] if lead else starts:
            for i in indices:
                copy(i).start()
        for copy in h_copies():
            copy.start()
        if lead:
            greet_all()
            tiles[me] = loss_ref[...]
            send_to_all(tiles, tile_send, tile_recv)
            for m in range(tokens // MT):
                turn_rb(m)
        else:
            greet_neighbours()

    def turn_rb(m):
        rbt[:, span(m, MT)] = rb_ref[span(m, MT), :].T

    def turn_h():
        whole = e_ref.at[:, pl.ds(h_base, NB)]
        pltpu.make_async_copy(whole, whole, h_sem).wait()
        for m in range(tokens // TILE):
            cols = span(m, TILE)
            for i in range(4):
                place = pl.multiple_of(h_base + i * 2 * rows_dev, 2 * rows_dev)
                flipped = e_ref[cols, pl.ds(place, 2 * rows_dev)].T
                ht[pl.ds(pl.multiple_of(i * rows_dev + core * mine, rows_dev), rows_dev), cols] = flipped[:rows_dev]
                ht[pl.ds(pl.multiple_of(i * rows_dev + (1 - core) * mine, rows_dev), rows_dev), cols] = flipped[rows_dev:]

    def core_copy(src, dst, send, recv):
        return pltpu.make_async_remote_copy(src_ref=src, dst_ref=dst, send_sem=send, recv_sem=recv, device_id=partner, device_id_type=MESH)

    def gi_core(turn):
        slot = parity(turn)
        return core_copy(gi_send.at[slot], gi_recv.at[slot], gi_dsend.at[slot], gi_drecv.at[slot])

    def outbox(piece):
        return piece & (go_send.shape[0] - 1)

    def go_core(piece):
        out, slot = outbox(piece), piece & 3
        return core_copy(go_send.at[out], go_recv.at[slot], go_dsend.at[out], go_drecv.at[slot])

    def ship(src, dst, i, sent, arrived, kept):
        if i < 3:
            pltpu.make_async_remote_copy(src_ref=src, dst_ref=dst(1 + i), send_sem=sent, recv_sem=arrived,
                                         device_id=(flip(me, 2 * OWNERS[i]),), device_id_type=MESH).start()
        else:
            pltpu.make_async_copy(src, dst(0), kept).start()

    def go_merge(piece):
        owner, part = piece & 3, piece >> 2
        rows = span(part, MT)
        go_core(piece).wait_recv()
        go_x[owner, rows, :] = go_x[owner, rows, :] + go_recv[piece & 3]
        ship(go_x.at[owner, rows], lambda slot: go_out.at[slot, rows], owner, go_sent.at[owner % 3], xrecv.at[3 + owner % 3], own_sem.at[1])

    def out_grad(owner, part, piece):
        rows = aligned(part, MT)
        total = rounded_sum(rbt[rows, :], a_buf[owner & (a_slots - 1)], half)

        @pl.when(core == 0)
        def _():
            go_x[owner, rows, :] = total[:, :unit]
            go_send[outbox(piece)] = total[:, unit:]

        @pl.when(core == 1)
        def _():
            go_x[owner, rows, :] = total[:, unit:]
            go_send[outbox(piece)] = total[:, :unit]

    def gi_merge(turn):
        gi_core(turn).wait_recv()
        gi_x[turn] = gi_x[turn] + gi_recv[parity(turn)]
        cols = hidden_cols(turn)
        for i in range(4):
            ship(gi_x.at[turn, pl.ds(i * rows_dev, rows_dev)], lambda slot: gi_out.at[slot, :, cols],
                 i, gi_sent.at[i % 3], xrecv.at[i % 3], own_sem.at[0])

    at(0, begin)
    turn = jnp.clip(step - lead, 0, TURNS - 1)
    working = (step >= lead) & (step < lead + TURNS)
    base = pl.multiple_of(chip_at(turn) * NB, NB)

    if lead:
        @pl.when(step < lead)
        def _():
            piece = jnp.minimum(step, 7)
            owner = piece & 3
            pl.when(piece < 4)(lambda: a_copy(owner).wait())
            pl.when(piece >= 4)(lambda: go_core(piece).wait_send())
            out_grad(owner, lax.shift_right_logical(piece, 2), piece)
        for p in range(8):
            at(p + 2, functools.partial(go_merge, p))
        pl.when(step < lead)(lambda: go_core(step).start())

    @pl.when(working)
    def _():
        @pl.when((step > lead) & (turn < TURNS - 1))
        def _():
            wo_copy(turn + 1).start()
            d_copy(turn + 1).start()
        wo_copy(turn).wait()
        d_copy(turn).wait()

    def slopes(turning):
        slot = parity(turn)
        for m in range(tokens // MT):
            rows = span(m, MT)
            u = lax.dot_general(rb_ref[rows, :], wo_buf[slot], NT, preferred_element_type=F32)
            e_ref[rows, pl.ds(base, NB)] = (d_buf[slot, rows, :] * u).astype(BF)
            if turning:
                turn_rb(m)

    if lead:
        pl.when(working)(lambda: slopes(False))
    else:
        at(0, lambda: slopes(True))
        pl.when(working & (step > 0))(lambda: slopes(False))

    at(lead, turn_h)

    if with_input_grad:
        def ahead():
            for i in range(2):
                wi_copy(jnp.int32(i)).start()
                r_copy(jnp.int32(i)).start()
        at(TURNS - 2, ahead)

        @pl.when(step >= TURNS)
        def _():
            index = jnp.maximum(step - TURNS, 0)
            block = halve(index)
            side = parity(index)

            @pl.when((index > 0) & (index < TAIL - 1))
            def _():
                r_copy(index + 1).start()

            @pl.when((side == 0) & (index > 0) & (index < TAIL - 2))
            def _():
                wi_copy(block + 1).start()
            pl.when(side == 0)(lambda: wi_copy(block).wait())
            r_copy(index).wait()
            for m in range(half // MT):
                rows = span(m, MT)
                left = e_ref[pl.ds(pl.multiple_of(side * half + m * MT, MT), MT), :]
                u = lax.dot_general(left, wi_buf[parity(block)], NT, preferred_element_type=F32) + r_buf[side, rows, :]
                rn_ref[rows, :] = u
                rbn_ref[rows, :] = u.astype(BF)

    pl.when((step >= lead + 2) & (step < lead + TURNS))(lambda: gi_core(turn).wait_send())

    @pl.when(working)
    def _():
        total = rounded_sum(ht[...], e_ref[:, pl.ds(base, NB)], half)
        gi_x[turn] = total[:mine]
        gi_send[parity(turn)] = total[mine:]

    last_merge = TURNS if with_input_grad else lead + TURNS - 1
    pl.when((step >= lead + 1) & (step <= last_merge))(lambda: gi_merge(jnp.clip(step - lead - 1, 0, TURNS - 1)))

    @pl.when(working)
    def _():
        gi_core(turn).start()

    if not lead:
        @pl.when(step < 4)
        def _():
            for i in range(2):
                piece = 2 * jnp.minimum(step, 3) + i
                owner = piece & 3
                a_copy(owner).wait()
                pl.when(step >= 1)(lambda: go_core(piece).wait_send())
                out_grad(owner, lax.shift_right_logical(piece, 2), piece)
                pl.when(step < 3)(lambda: a_copy((owner + 2) & 3).start())
        for p in range(8):
            at((p >> 1) + 1, functools.partial(go_merge, p))

        @pl.when(step < 4)
        def _():
            for part in range(2):
                go_core(2 * jnp.minimum(step, 3) + part).start()

    def end():
        if lead:
            gi_merge(TURNS - 1)
            loss_out[...] = sum_of_all(tiles, tile_send, tile_recv)
        for t in (TURNS - 2, TURNS - 1):
            gi_core(t).wait_send()
        for piece in range(go_send.shape[0]):
            go_core(piece).wait_send()
        for kind, sent, whole in ((0, gi_sent, gi_out.at[0]), (1, go_sent, go_out.at[0])):
            pltpu.make_async_copy(whole, whole, own_sem.at[kind]).wait()
            for i in range(3):
                pltpu.make_async_copy(whole, whole, sent.at[i]).wait()
                pltpu.make_async_copy(whole, whole, xrecv.at[3 * kind + i]).wait()
    at(TURNS + (TAIL if with_input_grad else LEAD) - 1, end)


def backward_layer(rb, r, h, w_in_full, w_out_full, a, d, with_input_grad, squares):
    tokens, width = rb.shape
    hidden = a.shape[1]
    half = tokens // 2
    rows_dev = width // DEVICES
    tail = lambda s: jnp.maximum(s - TURNS, 0)
    in_specs = [pl.BlockSpec((tokens, width), origin, pipeline_mode=pl.Buffered(1))] + [ANY] * 4
    args = [rb, w_out_full, a, d, h]
    out_specs, out_shape = [], []
    dma = pltpu.SemaphoreType.DMA
    two, three, four = dma((2,)), dma((3,)), dma((4,))
    small = (4 * rows_dev, NB)
    piece = (MT, NB // 2)
    scratch = [pltpu.VMEM((width, tokens), BF), pltpu.VMEM((8 * rows_dev, tokens), BF), pltpu.VMEM((tokens, hidden), BF),
               pltpu.VMEM((2, NB, width), BF), pltpu.VMEM((2 if with_input_grad else 4, tokens, NB), BF), pltpu.VMEM((2, tokens, NB), F32),
               pltpu.VMEM((TURNS,) + small, F32), pltpu.VMEM((2,) + small, F32), pltpu.VMEM((2,) + small, F32),
               pltpu.VMEM((4, width, NB // 2), F32), pltpu.VMEM((2 if with_input_grad else 4,) + piece, F32), pltpu.VMEM((4,) + piece, F32),
               dma, two, four, two, two, two, four, four, three, three, dma((6,)), two]
    if with_input_grad:
        block = lambda s: (tail(s) & 1, halve(tail(s)))
        in_specs += [ANY, ANY]
        args += [w_in_full, r]
        out_specs += [pl.BlockSpec((half, TILE), block)] * 2
        out_shape += [jax.ShapeDtypeStruct((tokens, width), F32), jax.ShapeDtypeStruct((tokens, width), BF)]
        scratch += [pltpu.VMEM((2, TILE, hidden), BF), pltpu.VMEM((2, half, TILE), F32), two, two]
    else:
        in_specs += [pl.BlockSpec(SUM_TILE, origin)]
        args += [squares]
        scratch += TILE_SCRATCH
    out_specs += [ANY, ANY]
    out_shape += [jax.ShapeDtypeStruct((4, rows_dev, hidden), F32), jax.ShapeDtypeStruct((4, width, hidden // DEVICES), F32)]
    if not with_input_grad:
        out_specs += [pl.BlockSpec(SUM_TILE, origin)]
        out_shape += [jax.ShapeDtypeStruct(SUM_TILE, F32)]
    return pl.pallas_call(
        functools.partial(backward_kernel, with_input_grad), grid=(TURNS + (TAIL if with_input_grad else LEAD),),
        in_specs=in_specs, out_specs=out_specs, out_shape=out_shape, scratch_shapes=scratch,
        compiler_params=pltpu.CompilerParams(collective_id=2 if with_input_grad else 3, has_side_effects=True, vmem_limit_bytes=VMEM_LIMIT),
        cost_estimate=pl.CostEstimate(flops=6 * tokens * width * hidden, bytes_accessed=100 * 2 ** 20, transcendentals=0),
        name='backward' if with_input_grad else 'backward_first')(*args)


class Parts:
    def __init__(self, layers, gi, go, w_in, w_out, vgi, vgo, vw_in, vw_out, sems):
        self.layers = layers
        self.copies = []
        for l in range(layers):
            for src, dst in ((gi[l], vgi.at[l]), (go[l], vgo.at[l]), (w_in.at[l], vw_in.at[l]), (w_out.at[l], vw_out.at[l])):
                self.copies.append((l, pltpu.make_async_copy(src, dst, sems.at[len(self.copies)])))
        self.vgi, self.vgo = vgi, vgo

    def start(self):
        for l in reversed(range(self.layers)):
            for layer, copy in self.copies:
                if layer == l:
                    copy.start()

    def wait(self, l):
        for layer, copy in self.copies:
            if layer == l:
                copy.wait()

    def each(self, l, use_in, use_out, carry):
        share = 1.0 / DEVICES

        def in_rows(i, c):
            rows = aligned(i, 8)
            total = self.vgi[l, 0, rows, :] + self.vgi[l, 1, rows, :] + self.vgi[l, 2, rows, :] + self.vgi[l, 3, rows, :]
            return use_in(rows, total * share, c)
        carry = lax.fori_loop(0, self.vgi.shape[2] // 8, in_rows, carry)

        def out_cols(i, c):
            rows = aligned(i, LANES)
            total = self.vgo[l, 0, rows, :] + self.vgo[l, 1, rows, :] + self.vgo[l, 2, rows, :] + self.vgo[l, 3, rows, :]
            return use_out(rows, (total * share).T, c)
        return lax.fori_loop(0, self.vgo.shape[2] // LANES, out_cols, carry)


def fold_squares(values):
    squares = values * values
    part = jnp.sum(squares.reshape(-1, 8, squares.shape[1]), axis=0)
    return sum(part[:, i:i + LANES] for i in range(0, part.shape[1], LANES))


def perturb_kernel(layers, radius, *refs):
    gi, go = refs[:layers], refs[layers:2 * layers]
    w_in, w_out = refs[2 * layers:2 * layers + 2]
    p_in, p_out = refs[2 * layers + 2:3 * layers + 2], refs[3 * layers + 2:4 * layers + 2]
    vgi, vgo, vw_in, vw_out, g_in, g_out, sems, tiles, send, recv = refs[4 * layers + 2:]
    parts = Parts(layers, gi, go, w_in, w_out, vgi, vgo, vw_in, vw_out, sems)
    parts.start()
    greet_all()
    total = jnp.zeros(SUM_TILE, F32)
    for l in reversed(range(layers)):
        parts.wait(l)

        def use_in(rows, mean, carry, l=l):
            g_in[l, rows, :] = mean
            return carry + fold_squares(mean)

        def use_out(rows, mean, carry, l=l):
            g_out[l, :, rows] = mean
            return carry + fold_squares(mean)
        total = parts.each(l, use_in, use_out, total)
    tiles[lax.axis_index('data')] = jnp.full(SUM_TILE, jnp.sum(total), F32)
    send_to_all(tiles, send, recv)
    norm = jnp.sqrt(sum_of_all(tiles, send, recv))
    scale = (radius / norm)[0:1, 0:1]
    for l in range(layers):
        def in_rows(i, carry, l=l):
            rows = aligned(i, 16)
            p_in[l][rows, :] = (vw_in[l, rows, :] + scale * g_in[l, rows, :]).astype(BF)
            return carry
        lax.fori_loop(0, p_in[l].shape[0] // 16, in_rows, 0)

        def out_rows(i, carry, l=l):
            rows = aligned(i, 64)
            p_out[l][rows, :] = (vw_out[l, rows, :] + scale * g_out[l, rows, :]).astype(BF)
            return carry
        lax.fori_loop(0, p_out[l].shape[0] // 64, out_rows, 0)


def update_kernel(layers, *refs):
    gi, go = refs[:layers], refs[layers:2 * layers]
    w_in, w_out, new_in, new_out, vgi, vgo, vw_in, vw_out, sems, done = refs[2 * layers:]
    parts = Parts(layers, gi, go, w_in, w_out, vgi, vgo, vw_in, vw_out, sems)
    parts.start()
    outs = []
    for l in reversed(range(layers)):
        parts.wait(l)

        def use_in(rows, mean, carry, l=l):
            vw_in[l, rows, :] = vw_in[l, rows, :] - LEARN_RATE * mean
            return carry

        def use_out(rows, mean, carry, l=l):
            vw_out[l, :, rows] = vw_out[l, :, rows] - LEARN_RATE * mean
            return carry
        parts.each(l, use_in, use_out, 0)
        for src, dst in ((vw_in.at[l], new_in.at[l]), (vw_out.at[l], new_out.at[l])):
            outs.append(pltpu.make_async_copy(src, dst, done.at[len(outs)]))
            outs[-1].start()
    for copy in outs:
        copy.wait()


def parts_scratch(gi, go, w_in, w_out):
    layers = len(gi)
    return [pltpu.VMEM((layers,) + gi[0].shape, F32), pltpu.VMEM((layers,) + go[0].shape, F32),
            pltpu.VMEM(w_in.shape, F32), pltpu.VMEM(w_out.shape, F32)]


def perturb(gi, go, w_in, w_out, radius):
    layers = len(gi)
    outs = [jax.ShapeDtypeStruct(w_in.shape[1:], BF)] * layers + [jax.ShapeDtypeStruct(w_out.shape[1:], BF)] * layers
    res = pl.pallas_call(
        functools.partial(perturb_kernel, layers, radius), out_shape=outs,
        in_specs=[ANY] * (2 * layers + 2), out_specs=[pl.BlockSpec(memory_space=pltpu.VMEM)] * (2 * layers),
        scratch_shapes=parts_scratch(gi, go, w_in, w_out) + [
            pltpu.VMEM(w_in.shape, F32), pltpu.VMEM(w_out.shape, F32), pltpu.SemaphoreType.DMA((4 * layers,))] + TILE_SCRATCH,
        compiler_params=pltpu.CompilerParams(collective_id=4, has_side_effects=True, vmem_limit_bytes=VMEM_LIMIT),
        name='perturb')(*gi, *go, w_in, w_out)
    return res[:layers], res[layers:]


def update(gi, go, w_in, w_out):
    layers = len(gi)
    return pl.pallas_call(
        functools.partial(update_kernel, layers),
        out_shape=[jax.ShapeDtypeStruct(w_in.shape, F32), jax.ShapeDtypeStruct(w_out.shape, F32)],
        in_specs=[ANY] * (2 * layers + 2), out_specs=[ANY, ANY],
        scratch_shapes=parts_scratch(gi, go, w_in, w_out) + [
            pltpu.SemaphoreType.DMA((4 * layers,)), pltpu.SemaphoreType.DMA((2 * layers,))],
        compiler_params=pltpu.CompilerParams(vmem_limit_bytes=VMEM_LIMIT), name='update')(*gi, *go, w_in, w_out)


def sam_pass(tokens, targets, shards_in, shards_out):
    layers = len(shards_in) if isinstance(shards_in, (list, tuple)) else shards_in.shape[0]
    if tokens.ndim == 2:
        full_in, full_out, tokens, *casts = gather_layer(shards_in, shards_out, tokens)
        shards_in, shards_out = casts[:layers], casts[layers:]
    else:
        full_in, full_out = gather_layer(shards_in[0], shards_out[0])
    h_cur = tokens.reshape(-1, tokens.shape[-1])
    saved = []
    for layer in range(layers):
        w_in_full = full_in.reshape(-1, full_in.shape[-1])
        if layer + 1 < layers:
            nxt = (shards_in[layer + 1], shards_out[layer + 1])
            wo, act, slope, h_next, full_in, full_out_next = forward_layer(h_cur, w_in_full, full_out, nxt)
        else:
            wo, act, slope, r, rb, squares, *other = forward_layer(h_cur, w_in_full, full_out, None, *targets)
            if other:
                targets = (targets[0], other[0])
        saved.append((h_cur, act, slope, w_in_full, wo.reshape(-1, wo.shape[-1])))
        if layer + 1 < layers:
            h_cur, full_out = h_next, full_out_next
    g_in = [None] * layers
    g_out = [None] * layers
    for layer in reversed(range(layers)):
        h_prev, act, slope, w_in_full, w_out_full = saved[layer]
        res = backward_layer(rb, r, h_prev, w_in_full, w_out_full, act, slope, layer > 0, squares)
        if layer > 0:
            r, rb, g_in[layer], g_out[layer] = res
        else:
            g_in[layer], g_out[layer], squares = res
    return squares, g_in, g_out, tokens, targets


def solution(mesh):
    groups = mesh.shape['data']
    batch, rows = P('data', None, None), P(None, 'data', None)

    def device_step(x_blk, y_blk, w_in_sh, w_out_sh):
        layers = w_in_sh.shape[0]
        model_dim = w_out_sh.shape[2]
        radius = RHO_FRAC * math.sqrt(layers * model_dim)
        x_tok = x_blk.reshape(-1, model_dim)
        y_tok = y_blk.reshape(-1, model_dim)
        _, g_in, g_out, x_pair, y_pair = sam_pass(x_tok, (y_tok,), w_in_sh, w_out_sh)
        pert_in, pert_out = perturb(g_in, g_out, w_in_sh, w_out_sh, radius)
        squares, gp_in, gp_out, _, _ = sam_pass(x_pair, y_pair, pert_in, pert_out)
        mean_loss = jnp.sum(squares) * (0.5 / (x_tok.shape[0] * groups))
        new_in, new_out = update(gp_in, gp_out, w_in_sh, w_out_sh)
        return new_in, new_out, mean_loss

    return jax.shard_map(device_step, mesh=mesh,
                         in_specs=(batch, batch, rows, rows), out_specs=(rows, rows, P()),
                         check_vma=False)
```
